32 devices in a mesh: pipe: 2 (over x), expert: 8 (over z, core), dp: 2 (over y).
Axes of the slice: x: 2, y: 2, z: 4, core: 2. Of those that a mesh axis runs over, the one named last changes fastest.
Arguments:
- tokens: bfloat16 [2, 2048, 2048], P('pipe', ('expert', 'dp')), may hold values from -6 to 6
- cotangent: bfloat16 [2, 2048, 2048], P('pipe', ('expert', 'dp')), may hold values from -6 to 6
- norm_gain: float32 [2, 2048], P('pipe'), may hold values from 0.5 to 1.5
- first_ids: int32 [2, 2048, 2], P('pipe', ('expert', 'dp')), may hold values from 0 to 3, all different within a row; in each aligned block of 128 rows (0 to 127, 128 to 255, ..., all dimensions but the last counted through in order) at most 72 rows name the same one
- first_gates: float32 [2, 2048, 2], P('pipe', ('expert', 'dp')), may hold values from 0.1 to 1
- second_ids: int32 [2, 2048, 2], P('pipe', ('expert', 'dp')), may hold values from 0 to 3, all different within a row; in each aligned block of 128 rows (0 to 127, 128 to 255, ..., all dimensions but the last counted through in order) at most 72 rows name the same one
- second_gates: float32 [2, 2048, 2], P('pipe', ('expert', 'dp')), may hold values from 0.1 to 1
- new_slot: int32 [2, 4], P('pipe'), may hold values from 0 to 3, each once within a row
- inner_weight: float32 [2, 8, 2, 2048, 384], P('pipe', 'expert', None, 'dp'), may hold values from -0.125 to 0.125
- outer_weight: float32 [2, 8, 384, 2048], P('pipe', 'expert', None, 'dp'), may hold values from -0.21875 to 0.21875
- inner_mean: bfloat16 [2, 8, 2, 2048, 384], P('pipe', 'expert', None, 'dp'), may hold values from -60 to 60
- outer_mean: bfloat16 [2, 8, 384, 2048], P('pipe', 'expert', None, 'dp'), may hold values from -60 to 60
- inner_square: bfloat16 [2, 8, 2, 2048, 384], P('pipe', 'expert', None, 'dp'), may hold values from 10 to 1000
- outer_square: bfloat16 [2, 8, 384, 2048], P('pipe', 'expert', None, 'dp'), may hold values from 10 to 1000
Outputs:
- layer_out: bfloat16 [2, 2048, 2048], P('pipe', ('expert', 'dp'))
- weight_inner: float32 [2, 8, 2, 2048, 384], P('pipe', 'expert', None, 'dp')
- weight_outer: float32 [2, 8, 384, 2048], P('pipe', 'expert', None, 'dp')
- mean_inner: bfloat16 [2, 8, 2, 2048, 384], P('pipe', 'expert', None, 'dp')
- mean_outer: bfloat16 [2, 8, 384, 2048], P('pipe', 'expert', None, 'dp')
- square_inner: bfloat16 [2, 8, 2, 2048, 384], P('pipe', 'expert', None, 'dp')
- square_outer: bfloat16 [2, 8, 384, 2048], P('pipe', 'expert', None, 'dp')
The draws below stay inside these ranges and needn't reach their ends.
Inputs may be any that keep to these rules, and one draw needn't show every extreme that they name: `first_ids`: each token names 2 different experts. Within the rows of one device no expert is named more than 72 times, and some device names some expert exactly 72 times. `second_ids`: as first_ids. `new_slot`: for each section, a permutation of the 4 experts.
All inputs are finite; a program needn't handle non-finite values.
Results may differ from the reference program's by a relative error of at most 0.008.
Values may be sent and summed in bfloat16 or wider, within the bound.
A program may use at most 128 MiB of HBM per device.

```python
import math
import jax
import jax.numpy as jnp
import numpy as np
from jax import lax

D = 2048
FF = 768
TOK_DEV = 128
EXPERTS = 4
TOPK = 2
CAP = 72
TOKENS = 2048
N_PIPE = 2
N_EXPERT = 8
N_DP = 2


def shard_levels(stream_key, extent, shards, least, largest):
    loudness, own = 1.0, jax.random.fold_in(stream_key, 6)
    for dim, shards_of in shards:
        draws = jnp.exp(jax.random.uniform(jax.random.fold_in(own, dim), (shards_of,), jnp.float32, least / len(shards), largest / len(shards)))
        loudness = loudness * jnp.repeat(draws, extent[dim] // shards_of).reshape([-1 if axis == dim else 1 for axis in range(len(extent))])
    return loudness


def routed_block(key, own, number, rows, count, top, reach, lean):
    sequence = jax.random.permutation(key, count)
    packed, ordinary = load_shares(count, rows * top, reach, lean, True), load_shares(count, rows * top, reach, lean, False)
    places = jnp.arange(count)

    def named(lengths, offset_by):
        used = int((lengths > 0).sum())
        fixed = max(1, used // 4)
        passed = fixed + (places - fixed + offset_by * (used - fixed)) % max(1, count - fixed)
        return jnp.zeros((count,), jnp.int32).at[sequence[jnp.where(places < fixed, places, passed)]].set(jnp.asarray(lengths, jnp.int32))

    lengths = jnp.where(number % 4 == 0, named(packed, number // 4), named(ordinary, number - number // 4 - 1))
    mixed = jax.random.permutation(jax.random.fold_in(own, 3), count)
    source_of, sink = mixed[0:count // 2 * 2:2], mixed[1:count // 2 * 2:2]
    margin = jnp.minimum(lengths[source_of] - 1, reach - lengths[sink]) // 2
    margin = jnp.where((source_of == sequence[0]) | (sink == sequence[0]) | (lengths[sink] == 0), 0, jnp.maximum(margin, 0))
    passed = jax.random.randint(jax.random.fold_in(own, 4), (count // 2,), 0, 1 << 20) % (margin + 1)
    lengths = lengths.at[source_of].add(-passed).at[sink].add(passed)
    items = jnp.searchsorted(jnp.cumsum(lengths), jnp.arange(rows * top), side="right").astype(jnp.int32)
    listing = items.reshape(top, rows).T
    listing = listing[jax.random.permutation(jax.random.fold_in(own, 1), rows)]
    offset_by = jax.random.randint(jax.random.fold_in(own, 2), (rows, 1), 0, top)
    return jnp.take_along_axis(listing, (jnp.arange(top)[None, :] + offset_by) % top, axis=1)


def load_shares(amount, total, bound, lean, full):
    portions = [(1 << 20) // math.isqrt(grade ** lean) + 1 for grade in range(1, amount + 1)]
    largest = bound if full else min(bound, max(-(-total // amount), total * portions[0] // sum(portions)))
    least = 1 if total - largest >= amount - 1 else 0
    given, rest = [largest] + [least] * (amount - 1), total - largest - least * (amount - 1)
    while rest > 0:
        movable = [i for i in range(1, amount) if given[i] < largest] or [i for i in range(1, amount) if given[i] < bound]
        mass, left = sum([portions[i] for i in movable]), rest
        for i in movable:
            more = min(bound - given[i], max(1, left * portions[i] // mass), rest)
            given[i] = given[i] + more
            rest = rest - more
    return np.array(given)


def centred(rng, extent, spread, bound, shards=(), held_as=jnp.bfloat16):
    entries = spread * jax.random.normal(rng, extent, jnp.float32)
    if shards:
        entries = entries * shard_levels(rng, extent, shards, -0.22, 0.18)
    return jnp.clip(entries, -bound, bound).astype(held_as)


def setup_inputs(seed: int = 0) -> dict:
    arg_keys = jax.random.split(jax.random.key(seed), 15)
    tokens = centred(arg_keys[0], (N_PIPE, TOKENS, D), 1.0, 6.0, ((0, 2), (1, 16)))
    cotangent = centred(arg_keys[1], (N_PIPE, TOKENS, D), 1.0, 6.0, ((0, 2), (1, 16)))
    norm_gain = jnp.clip(1.0 + 0.1 * jax.random.normal(arg_keys[2], (N_PIPE, D), jnp.float32), 0.5, 1.5)
    first_ids_keys = jax.random.split(jax.random.fold_in(arg_keys[3], 1), N_PIPE * TOKENS // TOK_DEV)
    first_ids_turns = jax.random.permutation(jax.random.fold_in(arg_keys[3], 3), N_PIPE * TOKENS // TOK_DEV)
    first_ids = jax.vmap(lambda own, number: routed_block(jax.random.fold_in(arg_keys[3], 2), own, number, TOK_DEV, EXPERTS, TOPK, CAP, 1))(first_ids_keys, first_ids_turns).reshape((N_PIPE, TOKENS, TOPK))
    first_gates = jnp.clip(0.1 + 0.9 * jax.random.uniform(arg_keys[4], (N_PIPE, TOKENS, TOPK), jnp.float32) ** shard_levels(arg_keys[4], (N_PIPE, TOKENS, TOPK), ((0, 2), (1, 16)), -0.2, 0.2), 0.1, 1.0)
    second_ids_keys = jax.random.split(jax.random.fold_in(arg_keys[5], 1), N_PIPE * TOKENS // TOK_DEV)
    second_ids_turns = jax.random.permutation(jax.random.fold_in(arg_keys[5], 3), N_PIPE * TOKENS // TOK_DEV)
    second_ids = jax.vmap(lambda own, number: routed_block(jax.random.fold_in(arg_keys[5], 2), own, number, TOK_DEV, EXPERTS, TOPK, CAP, 1))(second_ids_keys, second_ids_turns).reshape((N_PIPE, TOKENS, TOPK))
    second_gates = jnp.clip(0.1 + 0.9 * jax.random.uniform(arg_keys[6], (N_PIPE, TOKENS, TOPK), jnp.float32) ** shard_levels(arg_keys[6], (N_PIPE, TOKENS, TOPK), ((0, 2), (1, 16)), -0.2, 0.2), 0.1, 1.0)
    new_slot = jax.vmap(lambda own: jax.random.permutation(own, EXPERTS))(jax.random.split(arg_keys[7], N_PIPE)).reshape((N_PIPE, EXPERTS)).astype(jnp.int32)
    inner_weight = centred(arg_keys[8], (N_PIPE, 2 * EXPERTS, 2, D, FF // 2), D ** -0.5, 0.125, ((0, 2), (1, 8), (3, 2)), jnp.float32)
    outer_weight = centred(arg_keys[9], (N_PIPE, 2 * EXPERTS, FF // 2, D), FF ** -0.5, 0.21875, ((0, 2), (1, 8), (3, 2)), jnp.float32)
    inner_mean = centred(arg_keys[10], (N_PIPE, 2 * EXPERTS, 2, D, FF // 2), 10.0, 60.0, ((0, 2), (1, 8), (3, 2)))
    outer_mean = centred(arg_keys[11], (N_PIPE, 2 * EXPERTS, FF // 2, D), 10.0, 60.0, ((0, 2), (1, 8), (3, 2)))
    inner_square = jnp.clip(jnp.exp(math.log(1000.0) - 4.6051702 * jax.random.uniform(arg_keys[12], (N_PIPE, 2 * EXPERTS, 2, D, FF // 2), jnp.float32) ** shard_levels(arg_keys[12], (N_PIPE, 2 * EXPERTS, 2, D, FF // 2), ((0, 2), (1, 8), (3, 2)), -0.2, 0.2)), 10.0, 1000.0).astype(jnp.bfloat16)
    outer_square = jnp.clip(jnp.exp(math.log(1000.0) - 4.6051702 * jax.random.uniform(arg_keys[13], (N_PIPE, 2 * EXPERTS, FF // 2, D), jnp.float32) ** shard_levels(arg_keys[13], (N_PIPE, 2 * EXPERTS, FF // 2, D), ((0, 2), (1, 8), (3, 2)), -0.2, 0.2)), 10.0, 1000.0).astype(jnp.bfloat16)
    return {"tokens": tokens, "cotangent": cotangent, "norm_gain": norm_gain, "first_ids": first_ids, "first_gates": first_gates, "second_ids": second_ids, "second_gates": second_gates, "new_slot": new_slot, "inner_weight": inner_weight, "outer_weight": outer_weight, "inner_mean": inner_mean, "outer_mean": outer_mean, "inner_square": inner_square, "outer_square": outer_square}


norm_eps = 1e-06
learn_rate = 0.001
beta_one = 0.9
beta_two = 0.95
adam_eps = 1e-08
bias_one = 0.999973438601112
bias_two = 0.994079470779667

def normed(values, gain_row):
    widened = values.astype(jnp.float32)
    inverse_rms = lax.rsqrt(lax.optimization_barrier(jnp.mean(widened * widened, axis=-1, keepdims=True)) + norm_eps)
    return (widened * inverse_rms * gain_row).astype(jnp.bfloat16)

def silu_parts(gate_proj):
    logistic = jax.nn.sigmoid(gate_proj)
    return (gate_proj * logistic, logistic * (1.0 + gate_proj * (1.0 - logistic)))

def half_forward(token_rows, inner_full, outer_full):
    gate_proj = jnp.dot(token_rows, inner_full[0], preferred_element_type=jnp.float32)
    up_proj = jnp.dot(token_rows, inner_full[1], preferred_element_type=jnp.float32)
    activity = (silu_parts(gate_proj)[0] * up_proj).astype(jnp.bfloat16)
    half_out = jnp.dot(activity, outer_full, preferred_element_type=jnp.float32).astype(jnp.bfloat16)
    return (half_out, activity, gate_proj, up_proj)

def half_backward(token_rows, grad_rows, outer_full, activity, gate_proj, up_proj):
    grad_outer = jnp.dot(activity.T, grad_rows, preferred_element_type=jnp.float32)
    d_active = jnp.dot(grad_rows, outer_full.T, preferred_element_type=jnp.float32)
    swish_value, swish_slope = silu_parts(gate_proj)
    d_gate = (d_active * up_proj * swish_slope).astype(jnp.bfloat16)
    d_upper = (d_active * swish_value).astype(jnp.bfloat16)
    grad_gate = jnp.dot(token_rows.T, d_gate, preferred_element_type=jnp.float32)
    grad_upper = jnp.dot(token_rows.T, d_upper, preferred_element_type=jnp.float32)
    return (jnp.stack([grad_gate, grad_upper]), grad_outer)

def slot_rows(ids):
    blocked = ids.reshape(-1, TOK_DEV * TOPK)
    onehot = (blocked[..., None] == jnp.arange(EXPERTS, dtype=jnp.int32)).astype(jnp.int32)
    ranking = lax.optimization_barrier(jnp.sum((jnp.cumsum(onehot, axis=1) - 1) * onehot, axis=2)).astype(jnp.int32)
    starts = jnp.arange(blocked.shape[0], dtype=jnp.int32)[:, None] * CAP
    return (starts + ranking).reshape(ids.shape).astype(jnp.int32)

def scatter_rows(values, ids, positions):
    buffer = jnp.zeros((EXPERTS, TOKENS // TOK_DEV * CAP, D), jnp.bfloat16)
    return buffer.at[ids, positions].set(values)

def section_forward(token_rows, gain_row, ids, gates, inner_low, outer_low):
    normal = normed(token_rows, gain_row)
    positions = slot_rows(ids)
    buffer = scatter_rows(jnp.broadcast_to(normal[:, None, :], ids.shape + (D,)), ids, positions)
    totals = []
    stored = []
    for expert in range(EXPERTS):
        summed = jnp.zeros((buffer.shape[1], D), jnp.float32)
        for half_index in range(2):
            slot = 2 * expert + half_index
            half_out, activity, gate_proj, up_proj = half_forward(buffer[expert], inner_low[slot], outer_low[slot])
            summed = summed + lax.optimization_barrier(half_out).astype(jnp.float32)
            stored.append((activity, gate_proj, up_proj))
        totals.append(summed)
    totals = jnp.stack(totals)
    picked = totals[ids, positions]
    mixed_rows = token_rows.astype(jnp.float32) + lax.optimization_barrier(jnp.sum(gates[..., None] * picked, axis=1))
    return (mixed_rows.astype(jnp.bfloat16), buffer, stored)

def group_rows(values, dp_group):
    return values.reshape(N_EXPERT, N_DP, CAP, values.shape[-1])[:, dp_group].reshape(-1, values.shape[-1])

def section_grads(buffer, stored, grad_out, ids, gates, outer_low):
    positions = slot_rows(ids)
    grad_rows = (gates[..., None] * grad_out.astype(jnp.float32)[:, None, :]).astype(jnp.bfloat16)
    grad_buffer = scatter_rows(grad_rows, ids, positions)
    inner_list = []
    outer_list = []
    for expert in range(EXPERTS):
        for half_index in range(2):
            slot = 2 * expert + half_index
            activity, gate_proj, up_proj = stored[slot]
            total_inner = jnp.zeros((2, D, FF // 2), jnp.float32)
            total_outer = jnp.zeros((FF // 2, D), jnp.float32)
            for dp_group in range(N_DP):
                grad_inner, grad_outer = half_backward(group_rows(buffer[expert], dp_group), group_rows(grad_buffer[expert], dp_group), outer_low[slot], group_rows(activity, dp_group), group_rows(gate_proj, dp_group), group_rows(up_proj, dp_group))
                total_inner = total_inner + lax.optimization_barrier(grad_inner.astype(jnp.bfloat16)).astype(jnp.float32)
                total_outer = total_outer + lax.optimization_barrier(grad_outer.astype(jnp.bfloat16)).astype(jnp.float32)
            inner_list.append(total_inner)
            outer_list.append(total_outer)
    return (jnp.stack(inner_list), jnp.stack(outer_list))

def adam_step(weight, mean, square, grads):
    mean_new = (beta_one * mean.astype(jnp.float32) + (1.0 - beta_one) * grads).astype(jnp.bfloat16)
    square_new = (beta_two * square.astype(jnp.float32) + (1.0 - beta_two) * grads * grads).astype(jnp.bfloat16)
    mean_wide = lax.optimization_barrier(mean_new).astype(jnp.float32)
    square_wide = lax.optimization_barrier(square_new).astype(jnp.float32)
    update = mean_wide / bias_one / (jnp.sqrt(square_wide / bias_two) + adam_eps)
    return (weight - learn_rate * update, mean_new, square_new)

def reference(tokens, cotangent, norm_gain, first_ids, first_gates, second_ids, second_gates, new_slot, inner_weight, outer_weight, inner_mean, outer_mean, inner_square, outer_square):
    first_list = []
    inner_grads = []
    outer_grads = []
    for section in range(N_PIPE):
        inner_low = inner_weight[section].astype(jnp.bfloat16)
        outer_low = outer_weight[section].astype(jnp.bfloat16)
        section_out, buffer, stored = section_forward(tokens[section], norm_gain[section], first_ids[section], first_gates[section], inner_low, outer_low)
        grad_inner, grad_outer = section_grads(buffer, stored, cotangent[section], first_ids[section], first_gates[section], outer_low)
        first_list.append(section_out)
        inner_grads.append(grad_inner)
        outer_grads.append(grad_outer)
    first_out = lax.optimization_barrier(jnp.stack(first_list))
    second_in = jnp.roll(first_out, 1, axis=0)
    inner_new, inner_mean_new, inner_square_new = adam_step(inner_weight, inner_mean, inner_square, jnp.stack(inner_grads))
    outer_new, outer_mean_new, outer_square_new = adam_step(outer_weight, outer_mean, outer_square, jnp.stack(outer_grads))
    second_list = []
    for section in range(N_PIPE):
        section_out, buffer, stored = section_forward(second_in[section], norm_gain[section], second_ids[section], second_gates[section], inner_new[section].astype(jnp.bfloat16), outer_new[section].astype(jnp.bfloat16))
        second_list.append(section_out)
    layer_out = jnp.stack(second_list)
    sources = []
    halves = jnp.arange(2 * EXPERTS, dtype=jnp.int32)
    for section in range(N_PIPE):
        inverse = jnp.zeros((EXPERTS,), jnp.int32).at[new_slot[section]].set(jnp.arange(EXPERTS, dtype=jnp.int32))
        sources.append((2 * inverse[halves // 2] + halves % 2).astype(jnp.int32))

    def placed(array):
        return jnp.stack([array[section][sources[section]] for section in range(N_PIPE)])
    return (layer_out, placed(inner_new), placed(outer_new), placed(inner_mean_new), placed(outer_mean_new), placed(inner_square_new), placed(outer_square_new))
```

```python
import functools

import jax
import jax.numpy as jnp
from jax import lax
from jax.experimental import pallas as pl
from jax.experimental.pallas import tpu as pltpu
from jax.sharding import PartitionSpec as P

MESH = pl.DeviceIdType.MESH

norm_eps = 1e-06
learn_rate = 0.001
beta_one = 0.9
beta_two = 0.95
adam_eps = 1e-08
bias_one = 0.999973438601112
bias_two = 0.994079470779667


def for_sending(array):

    def short(part):
        return part.astype(jnp.bfloat16) if part.dtype == jnp.float32 else part

    return jax.tree.map(short, array)


def passed_along(block, axis, distance):
    devices = range(lax.axis_size(axis))
    route = [((i - distance) % len(devices), i) for i in devices]
    return lax.ppermute(block, axis, route)


def normed(values, gain_row):
    widened = values.astype(jnp.float32)
    inverse_rms = lax.rsqrt(jnp.mean(widened * widened, axis=-1, keepdims=True) + norm_eps)
    return (widened * inverse_rms * gain_row).astype(jnp.bfloat16)


def silu_parts(gate_proj):
    logistic = jax.nn.sigmoid(gate_proj)
    return (gate_proj * logistic, logistic * (1.0 + gate_proj * (1.0 - logistic)))


def half_forward(token_rows, inner_full, outer_full):
    gate_proj = jnp.dot(token_rows, inner_full[0], preferred_element_type=jnp.float32)
    up_proj = jnp.dot(token_rows, inner_full[1], preferred_element_type=jnp.float32)
    activity = (silu_parts(gate_proj)[0] * up_proj).astype(jnp.bfloat16)
    half_out = jnp.dot(activity, outer_full, preferred_element_type=jnp.float32).astype(
        jnp.bfloat16
    )
    return (half_out, activity, gate_proj, up_proj)


def half_backward(token_rows, grad_rows, outer_full, activity, gate_proj, up_proj):
    grad_outer = jnp.dot(activity.T, grad_rows, preferred_element_type=jnp.float32)
    d_active = jnp.dot(grad_rows, outer_full.T, preferred_element_type=jnp.float32)
    swish_value, swish_slope = silu_parts(gate_proj)
    d_gate = (d_active * up_proj * swish_slope).astype(jnp.bfloat16)
    d_upper = (d_active * swish_value).astype(jnp.bfloat16)
    grad_gate = jnp.dot(token_rows.T, d_gate, preferred_element_type=jnp.float32)
    grad_upper = jnp.dot(token_rows.T, d_upper, preferred_element_type=jnp.float32)
    return (jnp.stack([grad_gate, grad_upper]), grad_outer)


def slot_index(ids, pair_of, capacity):
    flattened = ids.reshape(-1)
    expert_row = jnp.arange(pair_of.shape[0], dtype=jnp.int32)
    onehot = (flattened[:, None] == expert_row[None, :]).astype(jnp.int32)
    ranking = jnp.sum((jnp.cumsum(onehot, axis=0) - 1) * onehot, axis=1)
    target = jnp.sum(onehot * pair_of[None, :], axis=1)
    return (target * capacity + ranking).reshape(ids.shape)


def selection(slots, values, total_slots):
    positions = jnp.arange(total_slots, dtype=jnp.int32)
    result = jnp.zeros((total_slots, slots.shape[0]), jnp.float32)
    for column in range(slots.shape[1]):
        result = result + jnp.where(
            slots[:, column][None, :] == positions[:, None], values[:, column][None, :], 0.0
        )
    return result


def across_chips(blocks):
    pairs = blocks.shape[0]
    groups = [[2 * pair + core for pair in range(pairs)] for core in range(2)]
    return lax.all_to_all(
        blocks, "expert", split_axis=0, concat_axis=0, tiled=True, axis_index_groups=groups
    )


def to_partner(block):
    devices = range(lax.axis_size("expert"))
    return lax.ppermute(block, "expert", [(i, i ^ 1) for i in devices])


def dispatched(packed, pair_count, capacity):
    own = across_chips(packed.reshape(pair_count, capacity, packed.shape[-1]))
    own = own.reshape(pair_count * capacity, -1)
    return jnp.concatenate([own, to_partner(own)], axis=0)


def gather_weights(inner_master, outer_master):
    inner_full, outer_full = (
        lax.all_gather(inner_master.astype(jnp.bfloat16), "dp", axis=3, tiled=True),
        lax.all_gather(outer_master.astype(jnp.bfloat16), "dp", axis=3, tiled=True),
    )
    return (inner_full[0, 0], outer_full[0, 0])


def pack_rows(token_rows, gain_row, ids, pair_of, capacity):
    pair_count = pair_of.shape[0]
    normal = normed(token_rows, gain_row)
    slots = slot_index(ids, pair_of, capacity)
    picker = selection(slots, jnp.ones(slots.shape, jnp.float32), pair_count * capacity).astype(
        jnp.bfloat16
    )
    packed = jnp.dot(picker, normal, preferred_element_type=jnp.float32).astype(jnp.bfloat16)
    return (slots, dispatched(packed, pair_count, capacity))


def returned_rows(token_rows, half_out, slots, gates, pair_count, capacity):
    rows = pair_count * capacity
    summed = half_out[:rows].astype(jnp.float32) + to_partner(half_out[rows:]).astype(jnp.float32)
    back = across_chips(summed.astype(jnp.bfloat16).reshape(pair_count, capacity, -1))
    weighting = selection(slots, gates, rows)
    mixed = lax.dot_general(
        weighting,
        back.reshape(rows, -1).astype(jnp.float32),
        (((0,), (0,)), ((), ())),
        precision=lax.Precision.HIGHEST,
    )
    return (token_rows.astype(jnp.float32) + mixed).astype(jnp.bfloat16)


def adam_step(weight, mean, square, grads):
    mean_new = (beta_one * mean.astype(jnp.float32) + (1.0 - beta_one) * grads).astype(jnp.bfloat16)
    square_new = (beta_two * square.astype(jnp.float32) + (1.0 - beta_two) * grads * grads).astype(
        jnp.bfloat16
    )
    mean_wide = lax.optimization_barrier(mean_new).astype(jnp.float32)
    square_wide = lax.optimization_barrier(square_new).astype(jnp.float32)
    update = mean_wide / bias_one / (jnp.sqrt(square_wide / bias_two) + adam_eps)
    return (weight - learn_rate * update, mean_new, square_new)


def crossing_counts(place):
    count = place.shape[-1]
    own = jnp.arange(count, dtype=jnp.int32)
    link = own[:-1, None]
    crosses = (own[None, :] <= link) & (place[..., None, :] > link)
    return jnp.sum(crosses.astype(jnp.int32), axis=-1)


def journey_rounds(place):
    count = place.shape[0]
    places = [place[i] for i in range(count)]

    def coloured(order, overlaps):
        rounds = [None] * count
        for position, item in enumerate(order):
            taken = [
                [overlaps(before, item) & (rounds[before] == r) for before in order[:position]]
                for r in range(count // 2)
            ]
            chosen = jnp.int32(0)
            for r in reversed(range(count // 2)):
                busy = functools.reduce(jnp.logical_or, taken[r], jnp.bool_(False))
                chosen = jnp.where(busy, chosen, r)
            rounds[item] = chosen
        return rounds

    up = coloured(list(range(count)), lambda b, i: (places[b] > i) & (places[i] > i))
    down = coloured(
        list(reversed(range(count))), lambda b, i: (places[b] < i) & (places[i] < i)
    )
    moved = [
        jnp.where(places[i] > i, up[i], jnp.where(places[i] < i, down[i], -1)) for i in range(count)
    ]
    return jnp.stack(moved)


def journey_flags(place, chip, this_round):
    count = place.shape[0]
    own = jnp.arange(count, dtype=jnp.int32)
    active = journey_rounds(place) == this_round
    starts = active & (own == chip)
    ends = active & (place == chip)
    up, down = place > own, place < own
    return jnp.stack(
        [jnp.any(starts & up), jnp.any(starts & down), jnp.any(ends & up), jnp.any(ends & down)]
    ).astype(jnp.int32)


def conveyor_kernel(chips, lag, pieces, flags, *refs):
    count = len(pieces)
    own = refs[:count]
    out = refs[count : 2 * count]
    up_in = refs[2 * count : 3 * count]
    down_in = refs[3 * count : 4 * count]
    up_out = refs[4 * count : 5 * count]
    down_out = refs[5 * count : 6 * count]
    up_sent, down_sent, up_got, down_got = refs[6 * count :]
    place = lax.axis_index("expert")
    chip = place // 2
    above, below = {"expert": place + 2}, {"expert": place - 2}
    has_above, has_below = chip < chips - 1, chip > 0

    barrier = pltpu.get_barrier_semaphore()

    @pl.when(has_above)
    def _():
        pl.semaphore_signal(barrier, inc=1, device_id=above, device_id_type=MESH)

    @pl.when(has_below)
    def _():
        pl.semaphore_signal(barrier, inc=1, device_id=below, device_id_type=MESH)

    pl.semaphore_wait(barrier, has_above.astype(jnp.int32) + has_below.astype(jnp.int32))

    start_up, start_down = flags[0] == 1, flags[1] == 1
    take_up, take_down = flags[2] == 1, flags[3] == 1
    total = sum(number for number, _ in pieces)

    def send(source, target, sent, got, k, index, device):
        pltpu.make_async_remote_copy(
            src_ref=source,
            dst_ref=target,
            send_sem=sent.at[k],
            recv_sem=got.at[index],
            device_id=device,
            device_id_type=MESH,
        ).start()

    def stream(index, first, last, onward, starting, arrived, leaving, sent, got):
        offset = 0
        for k, (number, rows) in enumerate(pieces):

            @pl.when((index >= offset) & (index < offset + number))
            def _(k=k, rows=rows, offset=offset):
                part = pl.ds(pl.multiple_of((index - offset) * rows, rows), rows)

                @pl.when(first)
                def _():
                    send(own[k].at[part], arrived[k].at[part], sent, got, k, index, onward)

                @pl.when(jnp.logical_not(first))
                def _():
                    pltpu.make_async_copy(
                        arrived[k].at[part], arrived[k].at[part], got.at[index]
                    ).wait()

                    @pl.when(jnp.logical_not(last))
                    def _():
                        leaving[k][part] = jnp.where(starting, own[k][part], arrived[k][part])
                        send(leaving[k].at[part], arrived[k].at[part], sent, got, k, index, onward)

            offset += number

    def settle(index):
        offset = 0
        for k, (number, rows) in enumerate(pieces):

            @pl.when((index >= offset) & (index < offset + number))
            def _(k=k, rows=rows, offset=offset):
                part = pl.ds(pl.multiple_of((index - offset) * rows, rows), rows)

                @pl.when(jnp.logical_not(has_below))
                def _():
                    out[k][part] = jnp.where(take_down, down_in[k][part], own[k][part])

                @pl.when(jnp.logical_not(has_above))
                def _():
                    out[k][part] = jnp.where(take_up, up_in[k][part], own[k][part])

                @pl.when(has_below & has_above)
                def _():
                    kept = jnp.where(take_down, down_in[k][part], own[k][part])
                    out[k][part] = jnp.where(take_up, up_in[k][part], kept)

            offset += number

    def step(t, carry):
        up_index = t - chip * lag
        down_index = t - (chips - 1 - chip) * lag
        stream(
            up_index, chip == 0, chip == chips - 1, above, start_up, up_in, up_out, up_sent, up_got
        )
        stream(
            down_index,
            chip == chips - 1,
            chip == 0,
            below,
            start_down,
            down_in,
            down_out,
            down_sent,
            down_got,
        )
        settle(jnp.minimum(up_index, down_index))
        return carry

    lax.fori_loop(0, total + (chips - 1) * lag, step, 0)

    for k in range(count):

        @pl.when(has_above)
        def _(k=k):
            pltpu.make_async_copy(up_in[k], up_in[k], up_sent.at[k]).wait()

        @pl.when(has_below)
        def _(k=k):
            pltpu.make_async_copy(down_in[k], down_in[k], down_sent.at[k]).wait()


def conveyed(arrays, flags, chips, lag, piece_bytes):
    pieces = []
    for array in arrays:
        row_bytes = array.shape[1] * 2
        rows = max(16, piece_bytes // row_bytes // 16 * 16)
        while array.shape[0] % rows:
            rows -= 16
        pieces.append((array.shape[0] // rows, rows))
    total = sum(number for number, _ in pieces)
    whole = [pltpu.VMEM(array.shape, array.dtype) for array in arrays]
    moved = sum(array.size * 2 for array in arrays)
    in_vmem = pl.BlockSpec(memory_space=pltpu.VMEM)
    return pl.pallas_call(
        functools.partial(conveyor_kernel, chips, lag, tuple(pieces)),
        out_shape=[jax.ShapeDtypeStruct(array.shape, array.dtype) for array in arrays],
        in_specs=[pl.BlockSpec(memory_space=pltpu.SMEM)] + [in_vmem] * len(arrays),
        out_specs=[in_vmem] * len(arrays),
        scratch_shapes=whole * 4
        + [
            pltpu.SemaphoreType.DMA((len(arrays),)),
            pltpu.SemaphoreType.DMA((len(arrays),)),
            pltpu.SemaphoreType.DMA((total,)),
            pltpu.SemaphoreType.DMA((total,)),
        ],
        compiler_params=pltpu.CompilerParams(
            collective_id=1, has_side_effects=True, vmem_limit_bytes=62 << 20
        ),
        cost_estimate=pl.CostEstimate(
            flops=100 * moved, bytes_accessed=2 * moved, transcendentals=0
        ),
    )(flags, *arrays)


def migrated(arrays, place, need):
    chips = place.shape[0]
    chip = lax.axis_index("expert") // 2
    flat = [array.reshape(-1, array.shape[-1]) for array in arrays]

    def one_round(this_round):
        flags = journey_flags(place, chip, this_round)
        return flags, conveyed(flat, flags, chips, 2, 98304)

    result = tuple(one_round(0)[1])
    for extra in range(1, chips // 2):

        def further(before, extra=extra):
            flags, moved = one_round(extra)
            taken = (flags[2] + flags[3]) > 0
            return tuple(jnp.where(taken, new, old) for new, old in zip(moved, before))

        result = lax.cond(need > extra, further, lambda before: before, result)
    return [new.reshape(array.shape) for new, array in zip(result, arrays)]


def per_device(
    tokens,
    cotangent,
    norm_gain,
    first_ids,
    first_gates,
    second_ids,
    second_gates,
    new_slot,
    inner_weight,
    outer_weight,
    inner_mean,
    outer_mean,
    inner_square,
    outer_square,
):
    pair_count = new_slot.shape[1]
    rows_here = tokens.shape[1]
    top_count = first_ids.shape[2]
    usual = rows_here * top_count // pair_count
    capacity = min(rows_here, usual + usual // 8)
    gain_row = norm_gain[0]
    homes = jnp.arange(pair_count, dtype=jnp.int32)
    need = lax.pmax(jnp.max(crossing_counts(new_slot[0])), "pipe")
    inner_full, outer_full = gather_weights(inner_weight, outer_weight)
    slots, arrived = pack_rows(tokens[0], gain_row, first_ids[0], homes, capacity)
    weighting = selection(slots, first_gates[0], pair_count * capacity)
    grad_packed = jnp.dot(
        weighting, cotangent[0].astype(jnp.float32), precision=lax.Precision.HIGHEST
    ).astype(jnp.bfloat16)
    grad_arrived = dispatched(grad_packed, pair_count, capacity)
    half_out, activity, gate_proj, up_proj = half_forward(arrived, inner_full, outer_full)
    grad_inner, grad_outer = half_backward(
        arrived, grad_arrived, outer_full, activity, gate_proj, up_proj
    )
    sum_inner, sum_outer = (
        lax.psum_scatter(
            grad_inner[None, None].astype(jnp.bfloat16), "dp", scatter_dimension=3, tiled=True
        ).astype(jnp.float32),
        lax.psum_scatter(
            grad_outer[None, None].astype(jnp.bfloat16), "dp", scatter_dimension=3, tiled=True
        ).astype(jnp.float32),
    )
    first_out = returned_rows(
        tokens[0], half_out, slots, first_gates[0], pair_count, capacity
    )
    new_inner, new_mean_in, new_square_in = adam_step(
        inner_weight, inner_mean, inner_square, sum_inner
    )
    new_outer, new_mean_out, new_square_out = adam_step(
        outer_weight, outer_mean, outer_square, sum_outer
    )
    low_inner, low_outer = for_sending((new_inner, new_outer))
    inner_two, outer_two = gather_weights(low_inner, low_outer)
    shifted = passed_along(first_out, "pipe", 1)
    slots_two, arrived_two = pack_rows(shifted, gain_row, second_ids[0], homes, capacity)
    moved = migrated(
        [low_outer, new_mean_out, new_square_out, low_inner, new_mean_in, new_square_in],
        new_slot[0],
        need,
    )
    half_two = half_forward(arrived_two, inner_two, outer_two)[0]
    second_out = returned_rows(
        shifted, half_two, slots_two, second_gates[0], pair_count, capacity
    )
    return (
        second_out[None],
        moved[3].astype(jnp.float32),
        moved[0].astype(jnp.float32),
        moved[4],
        moved[1],
        moved[5],
        moved[2],
    )


def solution(mesh):
    return jax.shard_map(
        per_device,
        mesh=mesh,
        in_specs=(
            P("pipe", ("expert", "dp"), None),
            P("pipe", ("expert", "dp"), None),
            P("pipe", None),
            P("pipe", ("expert", "dp"), None),
            P("pipe", ("expert", "dp"), None),
            P("pipe", ("expert", "dp"), None),
            P("pipe", ("expert", "dp"), None),
            P("pipe", None),
            P("pipe", "expert", None, "dp", None),
            P("pipe", "expert", None, "dp"),
            P("pipe", "expert", None, "dp", None),
            P("pipe", "expert", None, "dp"),
            P("pipe", "expert", None, "dp", None),
            P("pipe", "expert", None, "dp"),
        ),
        out_specs=(
            P("pipe", ("expert", "dp"), None),
            P("pipe", "expert", None, "dp", None),
            P("pipe", "expert", None, "dp"),
            P("pipe", "expert", None, "dp", None),
            P("pipe", "expert", None, "dp"),
            P("pipe", "expert", None, "dp", None),
            P("pipe", "expert", None, "dp"),
        ),
        check_vma=False,
    )
```

```python
import functools

import jax
import jax.numpy as jnp
from jax import lax
from jax.experimental import pallas as pl
from jax.experimental.pallas import tpu as pltpu
from jax.sharding import PartitionSpec as P


MESH = pl.DeviceIdType.MESH

norm_eps = 1e-06
learn_rate = 0.001
beta_one = 0.9
beta_two = 0.95
adam_eps = 1e-08
bias_one = 0.999973438601112
bias_two = 0.994079470779667


def for_sending(array):

    def short(part):
        return part.astype(jnp.bfloat16) if part.dtype == jnp.float32 else part

    return jax.tree.map(short, array)


def passed_along(block, axis, distance):
    devices = range(lax.axis_size(axis))
    route = [((i - distance) % len(devices), i) for i in devices]
    return lax.ppermute(block, axis, route)


def normed(values, gain_row):
    widened = values.astype(jnp.float32)
    inverse_rms = lax.rsqrt(jnp.mean(widened * widened, axis=-1, keepdims=True) + norm_eps)
    return (widened * inverse_rms * gain_row).astype(jnp.bfloat16)


def silu_parts(gate_proj):
    logistic = jax.nn.sigmoid(gate_proj)
    return (gate_proj * logistic, logistic * (1.0 + gate_proj * (1.0 - logistic)))


def columns(rows, part, parts):
    width = rows.shape[-1] // parts
    return rows[..., part * width : (part + 1) * width]


def half_forward(token_rows, inner_parts, outer_parts):
    count = len(inner_parts)

    def projected(which):
        return sum(
            jnp.dot(
                columns(token_rows, part, count),
                inner_parts[part][which],
                preferred_element_type=jnp.float32,
            )
            for part in range(count)
        )

    gate_proj, up_proj = projected(0), projected(1)
    activity = (silu_parts(gate_proj)[0] * up_proj).astype(jnp.bfloat16)
    half_out = [
        jnp.dot(activity, outer, preferred_element_type=jnp.float32).astype(jnp.bfloat16)
        for outer in outer_parts
    ]
    return (jnp.concatenate(half_out, axis=-1), activity, gate_proj, up_proj)


def half_backward(token_rows, grad_rows, outer_parts, activity, gate_proj, up_proj):
    count = len(outer_parts)

    def outer_part(part):
        return jnp.dot(
            activity.T, columns(grad_rows, part, count), preferred_element_type=jnp.float32
        ).astype(jnp.bfloat16)

    grad_outer = [outer_part(part) for part in range(count)]
    d_active = sum(
        jnp.dot(
            columns(grad_rows, part, count),
            outer_parts[part].T,
            preferred_element_type=jnp.float32,
        )
        for part in range(count)
    )
    swish_value, swish_slope = silu_parts(gate_proj)
    d_gate = (d_active * up_proj * swish_slope).astype(jnp.bfloat16)
    d_upper = (d_active * swish_value).astype(jnp.bfloat16)

    def inner_part(part):
        rows = columns(token_rows, part, count).T
        return jnp.stack(
            [
                jnp.dot(rows, d_gate, preferred_element_type=jnp.float32).astype(jnp.bfloat16),
                jnp.dot(rows, d_upper, preferred_element_type=jnp.float32).astype(jnp.bfloat16),
            ]
        )

    return ([inner_part(part) for part in range(count)], grad_outer)


def slot_index(ids, target, capacity):
    count, tokens = target.shape[0], ids.shape[0]
    experts = jnp.arange(count, dtype=jnp.int32)[None, :, None]
    chosen = (ids.T[:, None, :] == experts).astype(jnp.bfloat16)
    places = jnp.arange(tokens, dtype=jnp.int32)
    earlier = (places[:, None] < places[None, :]).astype(jnp.bfloat16)
    ranks = jnp.dot(
        chosen.reshape(-1, tokens), earlier, preferred_element_type=jnp.float32
    ).reshape(chosen.shape)
    chosen = chosen.astype(jnp.float32)
    totals = jnp.sum(chosen, axis=2, keepdims=True)
    before = jnp.cumsum(totals, axis=0) - totals
    starts = (target * capacity).astype(jnp.float32)[None, :, None]
    return jnp.sum(chosen * (starts + before + ranks), axis=1).astype(jnp.int32)


def selection(slots, values, total_slots):
    positions = jnp.arange(total_slots, dtype=jnp.int32)
    result = jnp.zeros((total_slots, slots.shape[1]), jnp.float32)
    for choice in range(slots.shape[0]):
        result = result + jnp.where(
            slots[choice][None, :] == positions[:, None], values[choice][None, :], 0.0
        )
    return result


def across_chips(blocks):
    devices = lax.axis_size("expert")
    arrived = [blocks[0]]
    for distance in range(1, len(blocks)):
        route = [(i, (i + 2 * distance) % devices) for i in range(devices)]
        arrived.append(lax.ppermute(blocks[distance], "expert", route))
    return arrived


def back_across_chips(blocks):
    devices = lax.axis_size("expert")
    arrived = [blocks[0]]
    for distance in range(1, len(blocks)):
        route = [(i, (i - 2 * distance) % devices) for i in range(devices)]
        arrived.append(lax.ppermute(blocks[distance], "expert", route))
    return arrived


def to_partner(block):
    devices = range(lax.axis_size("expert"))
    return lax.ppermute(block, "expert", [(i, i ^ 1) for i in devices])


def blocks_of(rows, count):
    size = rows.shape[0] // count
    return [rows[k * size : (k + 1) * size] for k in range(count)]


def dispatched(packed, pair_count):
    own = jnp.concatenate(across_chips(blocks_of(packed, pair_count)), axis=0)
    return jnp.concatenate([own, to_partner(own)], axis=0)


def from_ahead(block, axis, distance):
    return passed_along(block, axis, lax.axis_size(axis) - distance)


def turned(rows, back=False):
    share = rows.shape[-1] // lax.axis_size("dp")
    own = lax.axis_index("dp") * share
    return jnp.roll(rows, own if back else -own, axis=-1)


def gathered_parts(block):
    return [block] + [
        from_ahead(block, "dp", distance) for distance in range(1, lax.axis_size("dp"))
    ]


def summed_own(parts):
    total = parts[0].astype(jnp.float32)
    for distance in range(1, len(parts)):
        total = total + passed_along(parts[distance], "dp", distance).astype(jnp.float32)
    return total


def pack_rows(normal, slots, rows):
    picker = selection(slots, jnp.ones(slots.shape, jnp.float32), rows).astype(jnp.bfloat16)
    packed = jnp.dot(picker, normal, preferred_element_type=jnp.float32)
    return packed


def returned_rows(token_rows, half_out, slots, gates, pair_count):
    rows = half_out.shape[0] // 2
    other = to_partner(half_out[rows:])
    summed = (half_out[:rows].astype(jnp.float32) + other.astype(jnp.float32)).astype(jnp.bfloat16)
    back = jnp.concatenate(back_across_chips(blocks_of(summed, pair_count)), axis=0)
    weighting = selection(slots, gates, rows)
    high = weighting.astype(jnp.bfloat16)
    rest = (weighting - high.astype(jnp.float32)).astype(jnp.bfloat16)

    def weighted(share):
        return lax.dot_general(
            share, back, (((0,), (0,)), ((), ())), preferred_element_type=jnp.float32
        )

    mixed = weighted(high) + weighted(rest)
    return (token_rows.astype(jnp.float32) + mixed).astype(jnp.bfloat16)


def adam_step(weight, mean, square, grads):
    mean_new = (beta_one * mean.astype(jnp.float32) + (1.0 - beta_one) * grads).astype(jnp.bfloat16)
    square_new = (beta_two * square.astype(jnp.float32) + (1.0 - beta_two) * grads * grads).astype(
        jnp.bfloat16
    )
    mean_wide = lax.optimization_barrier(mean_new).astype(jnp.float32)
    square_wide = lax.optimization_barrier(square_new).astype(jnp.float32)
    update = mean_wide / bias_one / (jnp.sqrt(square_wide / bias_two) + adam_eps)
    return (weight - learn_rate * update, mean_new, square_new)


def crossing_counts(place):
    count = place.shape[-1]
    own = jnp.arange(count, dtype=jnp.int32)
    link = own[:-1, None]
    crosses = (own[None, :] <= link) & (place[..., None, :] > link)
    return jnp.sum(crosses.astype(jnp.int32), axis=-1)


def journey_flags(places, chip, this_round):
    count = len(places)

    def coloured(order, upward):
        moves = [(places[i] > i) if upward else (places[i] < i) for i in range(count)]
        rounds = [None] * count
        for position, item in enumerate(order):
            chosen = jnp.int32(0)
            for r in reversed(range(count // 2)):
                busy = jnp.bool_(False)
                for before in order[:position]:
                    passes = (places[before] > item) if upward else (places[before] < item)
                    busy = busy | (moves[before] & passes & (rounds[before] == r))
                chosen = jnp.where(busy, chosen, r)
            rounds[item] = chosen
        active = [moves[i] & (rounds[i] == this_round) for i in range(count)]
        starts, ends = jnp.bool_(False), jnp.bool_(False)
        for i in range(count):
            starts = starts | (active[i] & (chip == i))
            ends = ends | (active[i] & (places[i] == chip))
        return starts, ends

    start_up, take_up = coloured(list(range(count)), True)
    start_down, take_down = coloured(list(reversed(range(count))), False)
    return start_up, start_down, take_up, take_down


def conveyor_kernel(chips, lag, pieces, this_round, places, *refs):
    count = len(pieces)
    own = refs[:count]
    out = refs[count : 2 * count]
    up_in = refs[2 * count : 3 * count]
    down_in = refs[3 * count : 4 * count]
    up_out = refs[4 * count : 5 * count]
    down_out = refs[5 * count : 6 * count]
    up_sent, down_sent, up_got, down_got = refs[6 * count :]
    place = lax.axis_index("expert")
    chip = place // 2
    above, below = {"expert": place + 2}, {"expert": place - 2}
    has_above, has_below = chip < chips - 1, chip > 0

    barrier = pltpu.get_barrier_semaphore()

    @pl.when(has_above)
    def _():
        pl.semaphore_signal(barrier, inc=1, device_id=above, device_id_type=MESH)

    @pl.when(has_below)
    def _():
        pl.semaphore_signal(barrier, inc=1, device_id=below, device_id_type=MESH)

    pl.semaphore_wait(barrier, has_above.astype(jnp.int32) + has_below.astype(jnp.int32))

    start_up, start_down, take_up, take_down = journey_flags(
        [places[i] for i in range(chips)], chip, this_round
    )
    total = sum(number for number, _ in pieces)

    def send(source, target, sent, got, k, index, device):
        pltpu.make_async_remote_copy(
            src_ref=source,
            dst_ref=target,
            send_sem=sent.at[k],
            recv_sem=got.at[index],
            device_id=device,
            device_id_type=MESH,
        ).start()

    def stream(index, first, last, onward, starting, arrived, leaving, sent, got):
        offset = 0
        for k, (number, rows) in enumerate(pieces):

            @pl.when((index >= offset) & (index < offset + number))
            def _(k=k, rows=rows, offset=offset):
                part = pl.ds(pl.multiple_of((index - offset) * rows, rows), rows)

                @pl.when(first)
                def _():
                    send(own[k].at[part], arrived[k].at[part], sent, got, k, index, onward)

                @pl.when(jnp.logical_not(first))
                def _():
                    pltpu.make_async_copy(
                        arrived[k].at[part], arrived[k].at[part], got.at[index]
                    ).wait()

                    @pl.when(jnp.logical_not(last))
                    def _():
                        leaving[k][part] = jnp.where(starting, own[k][part], arrived[k][part])
                        send(leaving[k].at[part], arrived[k].at[part], sent, got, k, index, onward)

            offset += number

    def settle(index):
        offset = 0
        for k, (number, rows) in enumerate(pieces):

            @pl.when((index >= offset) & (index < offset + number))
            def _(k=k, rows=rows, offset=offset):
                part = pl.ds(pl.multiple_of((index - offset) * rows, rows), rows)

                @pl.when(jnp.logical_not(has_below))
                def _():
                    out[k][part] = jnp.where(take_down, down_in[k][part], own[k][part])

                @pl.when(jnp.logical_not(has_above))
                def _():
                    out[k][part] = jnp.where(take_up, up_in[k][part], own[k][part])

                @pl.when(has_below & has_above)
                def _():
                    kept = jnp.where(take_down, down_in[k][part], own[k][part])
                    out[k][part] = jnp.where(take_up, up_in[k][part], kept)

            offset += number

    def step(t, carry):
        up_index = t - chip * lag
        down_index = t - (chips - 1 - chip) * lag
        stream(
            up_index, chip == 0, chip == chips - 1, above, start_up, up_in, up_out, up_sent, up_got
        )
        stream(
            down_index,
            chip == chips - 1,
            chip == 0,
            below,
            start_down,
            down_in,
            down_out,
            down_sent,
            down_got,
        )
        settle(jnp.minimum(up_index, down_index))
        return carry

    lax.fori_loop(0, total + (chips - 1) * lag, step, 0)

    for k in range(count):

        @pl.when(has_above)
        def _(k=k):
            pltpu.make_async_copy(up_in[k], up_in[k], up_sent.at[k]).wait()

        @pl.when(has_below)
        def _(k=k):
            pltpu.make_async_copy(down_in[k], down_in[k], down_sent.at[k]).wait()


def conveyed(arrays, place, this_round, lag, piece_bytes):
    chips = place.shape[0]
    pieces = []
    for array in arrays:
        row_bytes = array.shape[1] * 2
        rows = max(16, piece_bytes // row_bytes // 16 * 16)
        while array.shape[0] % rows:
            rows -= 16
        pieces.append((array.shape[0] // rows, rows))
    total = sum(number for number, _ in pieces)
    whole = [pltpu.VMEM(array.shape, array.dtype) for array in arrays]
    moved = sum(array.size * 2 for array in arrays)
    in_vmem = pl.BlockSpec(memory_space=pltpu.VMEM)
    return pl.pallas_call(
        functools.partial(conveyor_kernel, chips, lag, tuple(pieces), this_round),
        out_shape=[jax.ShapeDtypeStruct(array.shape, array.dtype) for array in arrays],
        in_specs=[pl.BlockSpec(memory_space=pltpu.SMEM)] + [in_vmem] * len(arrays),
        out_specs=[in_vmem] * len(arrays),
        scratch_shapes=whole * 4
        + [
            pltpu.SemaphoreType.DMA((len(arrays),)),
            pltpu.SemaphoreType.DMA((len(arrays),)),
            pltpu.SemaphoreType.DMA((total,)),
            pltpu.SemaphoreType.DMA((total,)),
        ],
        compiler_params=pltpu.CompilerParams(
            collective_id=1 + this_round, has_side_effects=True, vmem_limit_bytes=62 << 20
        ),
        cost_estimate=pl.CostEstimate(
            flops=100 * moved, bytes_accessed=2 * moved, transcendentals=0
        ),
    )(place, *arrays)


def first_journey(arrays, place):
    flat = [array.reshape(-1, array.shape[-1]) for array in arrays]
    return flat, tuple(conveyed(flat, place, 0, 2, 98304))


def further_journeys(flat, result, place, need):
    chips = place.shape[0]
    chip = lax.axis_index("expert") // 2

    def rounds_from(this_round, before):
        if this_round == chips // 2:
            return before

        def further(before):
            _, _, take_up, take_down = journey_flags(
                [place[i] for i in range(chips)], chip, this_round
            )
            moved = conveyed(flat, place, this_round, 2, 98304)
            merged = tuple(
                jnp.where(take_up | take_down, new, old) for new, old in zip(moved, before)
            )
            return rounds_from(this_round + 1, merged)

        return lax.cond(need > this_round, further, lambda before: before, before)

    return rounds_from(1, result)


def whole_step(
    tokens,
    cotangent,
    norm_gain,
    first_ids,
    first_gates,
    second_ids,
    second_gates,
    new_slot,
    inner_weight,
    outer_weight,
    inner_mean,
    outer_mean,
    inner_square,
    outer_square,
):
    pair_count = new_slot.shape[1]
    rows_here = tokens.shape[1]
    top_count = first_ids.shape[2]
    usual = rows_here * top_count // pair_count
    capacity = min(rows_here, usual + usual // 8)
    rows = pair_count * capacity
    chip = lax.axis_index("expert") // 2
    ahead = (jnp.arange(pair_count, dtype=jnp.int32) - chip) % pair_count
    need = jnp.max(crossing_counts(new_slot[0]))
    for distance in range(1, lax.axis_size("pipe")):
        need = jnp.maximum(
            need, jnp.max(crossing_counts(passed_along(new_slot, "pipe", distance)[0]))
        )
    inner_parts = gathered_parts(inner_weight[0, 0].astype(jnp.bfloat16))
    outer_parts = gathered_parts(outer_weight[0, 0].astype(jnp.bfloat16))
    gain_row = turned(norm_gain[0])
    token_rows = turned(tokens[0])
    slots = slot_index(first_ids[0], ahead, capacity)
    packed = pack_rows(normed(token_rows, gain_row), slots, rows).astype(jnp.bfloat16)
    arrived = dispatched(packed, pair_count)
    gates = first_gates[0].T
    slot_gates = jnp.sum(selection(slots, gates, rows), axis=1, keepdims=True)
    grad_packed = (pack_rows(turned(cotangent[0]), slots, rows) * slot_gates).astype(jnp.bfloat16)
    grad_arrived = dispatched(grad_packed, pair_count)
    half_out, *kept = half_forward(arrived, inner_parts, outer_parts)
    activity, gate_proj, up_proj = lax.optimization_barrier(kept)
    grad_inner, grad_outer = half_backward(
        arrived, grad_arrived, outer_parts, activity, gate_proj, up_proj
    )
    sum_inner = summed_own(grad_inner)
    sum_outer = summed_own(grad_outer)
    first_out = returned_rows(token_rows, half_out, slots, gates, pair_count)
    shifted = passed_along(first_out, "pipe", 1)
    new_inner, new_mean_in, new_square_in = adam_step(
        inner_weight[0, 0], inner_mean[0, 0], inner_square[0, 0], sum_inner
    )
    new_outer, new_mean_out, new_square_out = adam_step(
        outer_weight[0, 0], outer_mean[0, 0], outer_square[0, 0], sum_outer
    )
    low_inner, low_outer = for_sending((new_inner, new_outer))
    inner_two, outer_two = gathered_parts(low_inner), gathered_parts(low_outer)
    slots_two = slot_index(second_ids[0], ahead, capacity)
    packed_two = pack_rows(normed(shifted, gain_row), slots_two, rows).astype(jnp.bfloat16)
    stepped = (low_outer, new_mean_out, new_square_out, low_inner, new_mean_in, new_square_in)
    packed_two, need = lax.optimization_barrier((packed_two, need))
    arrived_two = dispatched(packed_two, pair_count)
    stepped, arrived_two = lax.optimization_barrier((stepped, arrived_two))
    flat, moved = first_journey(stepped, new_slot[0])
    moved, arrived_two, inner_two, outer_two = lax.optimization_barrier(
        (moved, arrived_two, inner_two, outer_two)
    )
    half_two = half_forward(arrived_two, inner_two, outer_two)[0]
    second_out = turned(
        returned_rows(shifted, half_two, slots_two, second_gates[0].T, pair_count),
        back=True,
    )
    moved = further_journeys(flat, moved, new_slot[0], need)
    moved = [
        jnp.where(need < 0, 0.0, array.astype(jnp.float32)).astype(
            jnp.bfloat16 if position % 3 else jnp.float32
        )
        for position, array in enumerate(moved)
    ]
    outer_shape, inner_shape = outer_weight.shape, inner_weight.shape
    return (
        second_out[None],
        moved[3].reshape(inner_shape),
        moved[0].reshape(outer_shape),
        moved[4].reshape(inner_shape),
        moved[1].reshape(outer_shape),
        moved[5].reshape(inner_shape),
        moved[2].reshape(outer_shape),
    )


def solution(mesh):
    return jax.shard_map(
        whole_step,
        mesh=mesh,
        in_specs=(
            P("pipe", ("expert", "dp"), None),
            P("pipe", ("expert", "dp"), None),
            P("pipe", None),
            P("pipe", ("expert", "dp"), None),
            P("pipe", ("expert", "dp"), None),
            P("pipe", ("expert", "dp"), None),
            P("pipe", ("expert", "dp"), None),
            P("pipe", None),
            P("pipe", "expert", None, "dp", None),
            P("pipe", "expert", None, "dp"),
            P("pipe", "expert", None, "dp", None),
            P("pipe", "expert", None, "dp"),
            P("pipe", "expert", None, "dp", None),
            P("pipe", "expert", None, "dp"),
        ),
        out_specs=(
            P("pipe", ("expert", "dp"), None),
            P("pipe", "expert", None, "dp", None),
            P("pipe", "expert", None, "dp"),
            P("pipe", "expert", None, "dp", None),
            P("pipe", "expert", None, "dp"),
            P("pipe", "expert", None, "dp", None),
            P("pipe", "expert", None, "dp"),
        ),
        check_vma=False,
    )
```

```python
import functools

import jax
import jax.numpy as jnp
from jax import lax
from jax.experimental import pallas as pl
from jax.experimental.pallas import tpu as pltpu
from jax.sharding import PartitionSpec as P


MESH = pl.DeviceIdType.MESH

norm_eps = 1e-06
learn_rate = 0.001
beta_one = 0.9
beta_two = 0.95
adam_eps = 1e-08
bias_one = 0.999973438601112
bias_two = 0.994079470779667
LAG = 2
PIECE = 98304


def for_sending(array):

    def short(part):
        return part.astype(jnp.bfloat16) if part.dtype == jnp.float32 else part

    return jax.tree.map(short, array)


def passed_along(block, axis, distance):
    devices = range(lax.axis_size(axis))
    route = [((i - distance) % len(devices), i) for i in devices]
    return lax.ppermute(block, axis, route)


def normed(values, gain_row):
    widened = values.astype(jnp.float32)
    inverse_rms = lax.rsqrt(jnp.mean(widened * widened, axis=-1, keepdims=True) + norm_eps)
    return (widened * inverse_rms * gain_row).astype(jnp.bfloat16)


def silu_parts(gate_proj):
    logistic = jax.nn.sigmoid(gate_proj)
    return (gate_proj * logistic, logistic * (1.0 + gate_proj * (1.0 - logistic)))


def columns(rows, part, parts):
    width = rows.shape[-1] // parts
    return rows[..., part * width : (part + 1) * width]


def half_forward(token_rows, inner_parts, outer_parts):
    count = len(inner_parts)

    def projected(which):
        return sum(
            jnp.dot(
                columns(token_rows, part, count),
                inner_parts[part][which],
                preferred_element_type=jnp.float32,
            )
            for part in range(count)
        )

    gate_proj, up_proj = projected(0), projected(1)
    activity = (silu_parts(gate_proj)[0] * up_proj).astype(jnp.bfloat16)

    def half_out(rows):
        return jnp.concatenate(
            [
                jnp.dot(rows, outer, preferred_element_type=jnp.float32).astype(jnp.bfloat16)
                for outer in outer_parts
            ],
            axis=-1,
        )

    middle = activity.shape[0] // 2
    for_partner = half_out(activity[middle:])
    for_own = half_out(activity[:middle])
    return ((for_own, for_partner), activity, gate_proj, up_proj)


def half_backward(token_rows, grad_rows, outer_parts, activity, gate_proj, up_proj):
    count = len(outer_parts)

    def outer_part(part):
        return jnp.dot(
            activity.T, columns(grad_rows, part, count), preferred_element_type=jnp.float32
        ).astype(jnp.bfloat16)

    grad_outer = [outer_part(part) for part in range(count)]
    d_active = sum(
        jnp.dot(
            columns(grad_rows, part, count),
            outer_parts[part].T,
            preferred_element_type=jnp.float32,
        )
        for part in range(count)
    )
    swish_value, swish_slope = silu_parts(gate_proj)
    d_gate = (d_active * up_proj * swish_slope).astype(jnp.bfloat16)
    d_upper = (d_active * swish_value).astype(jnp.bfloat16)

    def inner_part(part):
        rows = columns(token_rows, part, count).T
        return jnp.stack(
            [
                jnp.dot(rows, d_gate, preferred_element_type=jnp.float32).astype(jnp.bfloat16),
                jnp.dot(rows, d_upper, preferred_element_type=jnp.float32).astype(jnp.bfloat16),
            ]
        )

    return ([inner_part(part) for part in range(count)], grad_outer)


def slot_index(ids, target, capacity):
    count, tokens = target.shape[0], ids.shape[0]
    experts = jnp.arange(count, dtype=jnp.int32)[None, :, None]
    chosen = (ids.T[:, None, :] == experts).astype(jnp.bfloat16)
    places = jnp.arange(tokens, dtype=jnp.int32)
    earlier = (places[:, None] < places[None, :]).astype(jnp.bfloat16)
    ranks = jnp.dot(
        chosen.reshape(-1, tokens), earlier, preferred_element_type=jnp.float32
    ).reshape(chosen.shape)
    chosen = chosen.astype(jnp.float32)
    totals = jnp.sum(chosen, axis=2, keepdims=True)
    before = jnp.cumsum(totals, axis=0) - totals
    starts = (target * capacity).astype(jnp.float32)[None, :, None]
    return jnp.sum(chosen * (starts + before + ranks), axis=1).astype(jnp.int32)


def selection(slots, values, total_slots):
    positions = jnp.arange(total_slots, dtype=jnp.int32)
    result = jnp.zeros((total_slots, slots.shape[1]), jnp.float32)
    for choice in range(slots.shape[0]):
        result = result + jnp.where(
            slots[choice][None, :] == positions[:, None], values[choice][None, :], 0.0
        )
    return result


def across_chips(blocks):
    devices = lax.axis_size("expert")
    arrived = [blocks[0]]
    for distance in range(1, len(blocks)):
        route = [(i, (i + 2 * distance) % devices) for i in range(devices)]
        arrived.append(lax.ppermute(blocks[distance], "expert", route))
    return arrived


def back_across_chips(blocks):
    devices = lax.axis_size("expert")
    arrived = [blocks[0]]
    for distance in range(1, len(blocks)):
        route = [(i, (i - 2 * distance) % devices) for i in range(devices)]
        arrived.append(lax.ppermute(blocks[distance], "expert", route))
    return arrived


def to_partner(block):
    devices = range(lax.axis_size("expert"))
    return lax.ppermute(block, "expert", [(i, i ^ 1) for i in devices])


def blocks_of(rows, count):
    size = rows.shape[0] // count
    return [rows[k * size : (k + 1) * size] for k in range(count)]


def dispatched(packed, pair_count):
    own = jnp.concatenate(across_chips(blocks_of(packed, pair_count)), axis=0)
    return jnp.concatenate([own, to_partner(own)], axis=0)


def from_ahead(block, axis, distance):
    return passed_along(block, axis, lax.axis_size(axis) - distance)


def turned(rows, back=False):
    share = rows.shape[-1] // lax.axis_size("dp")
    own = lax.axis_index("dp") * share
    return jnp.roll(rows, own if back else -own, axis=-1)


def gathered_parts(block):
    return [block] + [
        from_ahead(block, "dp", distance) for distance in range(1, lax.axis_size("dp"))
    ]


def summed_own(parts):
    total = parts[0].astype(jnp.float32)
    for distance in range(1, len(parts)):
        total = total + passed_along(parts[distance], "dp", distance).astype(jnp.float32)
    return total


def pack_rows(normal, slots, rows):
    picker = selection(slots, jnp.ones(slots.shape, jnp.float32), rows).astype(jnp.bfloat16)
    packed = jnp.dot(picker, normal, preferred_element_type=jnp.float32)
    return packed


def returned_rows(token_rows, half_out, slots, gates, pair_count):
    for_own, for_partner = half_out
    rows = for_own.shape[0]
    other = to_partner(for_partner)
    summed = (for_own.astype(jnp.float32) + other.astype(jnp.float32)).astype(jnp.bfloat16)
    back = jnp.concatenate(back_across_chips(blocks_of(summed, pair_count)), axis=0)
    weighting = selection(slots, gates, rows)
    high = weighting.astype(jnp.bfloat16)
    rest = (weighting - high.astype(jnp.float32)).astype(jnp.bfloat16)

    def weighted(share):
        return lax.dot_general(
            share, back, (((0,), (0,)), ((), ())), preferred_element_type=jnp.float32
        )

    mixed = weighted(high) + weighted(rest)
    return (token_rows.astype(jnp.float32) + mixed).astype(jnp.bfloat16)


def adam_step(weight, mean, square, grads):
    mean_new = (beta_one * mean.astype(jnp.float32) + (1.0 - beta_one) * grads).astype(jnp.bfloat16)
    square_new = (beta_two * square.astype(jnp.float32) + (1.0 - beta_two) * grads * grads).astype(
        jnp.bfloat16
    )
    mean_wide = lax.optimization_barrier(mean_new).astype(jnp.float32)
    square_wide = lax.optimization_barrier(square_new).astype(jnp.float32)
    update = mean_wide / bias_one / (jnp.sqrt(square_wide / bias_two) + adam_eps)
    return (weight - learn_rate * update, mean_new, square_new)


def crossing_counts(place):
    count = place.shape[-1]
    own = jnp.arange(count, dtype=jnp.int32)
    link = own[:-1, None]
    crosses = (own[None, :] <= link) & (place[..., None, :] > link)
    return jnp.sum(crosses.astype(jnp.int32), axis=-1)


def journey_flags(places, chip, this_round):
    count = len(places)

    def coloured(order, upward):
        moves = [(places[i] > i) if upward else (places[i] < i) for i in range(count)]
        rounds = [None] * count
        for position, item in enumerate(order):
            chosen = jnp.int32(0)
            for r in reversed(range(count // 2)):
                busy = jnp.bool_(False)
                for before in order[:position]:
                    passes = (places[before] > item) if upward else (places[before] < item)
                    busy = busy | (moves[before] & passes & (rounds[before] == r))
                chosen = jnp.where(busy, chosen, r)
            rounds[item] = chosen
        active = [moves[i] & (rounds[i] == this_round) for i in range(count)]
        starts, ends = jnp.bool_(False), jnp.bool_(False)
        for i in range(count):
            starts = starts | (active[i] & (chip == i))
            ends = ends | (active[i] & (places[i] == chip))
        return starts, ends

    start_up, take_up = coloured(list(range(count)), True)
    start_down, take_down = coloured(list(reversed(range(count))), False)
    return start_up, start_down, take_up, take_down


def conveyor_kernel(chips, lag, pieces, this_round, places, *refs):
    count = len(pieces)
    source = refs[:count]
    result = refs[count : 2 * count]
    own = refs[2 * count : 3 * count]
    out = refs[3 * count : 4 * count]
    up_in = refs[4 * count : 5 * count]
    down_in = refs[5 * count : 6 * count]
    up_out = refs[6 * count : 7 * count]
    down_out = refs[7 * count : 8 * count]
    loaded, stored, up_sent, down_sent, up_got, down_got = refs[8 * count :]
    place = lax.axis_index("expert")
    chip = place // 2
    above, below = {"expert": place + 2}, {"expert": place - 2}
    has_above, has_below = chip < chips - 1, chip > 0

    offset = 0
    for k, (number, rows) in enumerate(pieces):

        def load(i, carry, k=k, rows=rows, offset=offset):
            part = pl.ds(pl.multiple_of(i * rows, rows), rows)
            pltpu.make_async_copy(source[k].at[part], own[k].at[part], loaded.at[offset + i]).start()
            return carry

        lax.fori_loop(0, number, load, 0)
        offset += number

    barrier = pltpu.get_barrier_semaphore()

    @pl.when(has_above)
    def _():
        pl.semaphore_signal(barrier, inc=1, device_id=above, device_id_type=MESH)

    @pl.when(has_below)
    def _():
        pl.semaphore_signal(barrier, inc=1, device_id=below, device_id_type=MESH)

    pl.semaphore_wait(barrier, has_above.astype(jnp.int32) + has_below.astype(jnp.int32))

    start_up, start_down, take_up, take_down = journey_flags(
        [places[i] for i in range(chips)], chip, this_round
    )
    total = sum(number for number, _ in pieces)

    def send(block, target, sent, got, k, index, device):
        pltpu.make_async_remote_copy(
            src_ref=block,
            dst_ref=target,
            send_sem=sent.at[k],
            recv_sem=got.at[index],
            device_id=device,
            device_id_type=MESH,
        ).start()

    def stream(index, first, last, onward, starting, arrived, leaving, sent, got):
        offset = 0
        for k, (number, rows) in enumerate(pieces):

            @pl.when((index >= offset) & (index < offset + number))
            def _(k=k, rows=rows, offset=offset):
                part = pl.ds(pl.multiple_of((index - offset) * rows, rows), rows)

                @pl.when(first)
                def _():
                    send(own[k].at[part], arrived[k].at[part], sent, got, k, index, onward)

                @pl.when(jnp.logical_not(first))
                def _():
                    pltpu.make_async_copy(
                        arrived[k].at[part], arrived[k].at[part], got.at[index]
                    ).wait()

                    @pl.when(jnp.logical_not(last))
                    def _():
                        leaving[k][part] = jnp.where(starting, own[k][part], arrived[k][part])
                        send(leaving[k].at[part], arrived[k].at[part], sent, got, k, index, onward)

            offset += number

    def settle(index):
        offset = 0
        for k, (number, rows) in enumerate(pieces):

            @pl.when((index >= offset) & (index < offset + number))
            def _(k=k, rows=rows, offset=offset):
                part = pl.ds(pl.multiple_of((index - offset) * rows, rows), rows)

                @pl.when(jnp.logical_not(has_below))
                def _():
                    out[k][part] = jnp.where(take_down, down_in[k][part], own[k][part])

                @pl.when(jnp.logical_not(has_above))
                def _():
                    out[k][part] = jnp.where(take_up, up_in[k][part], own[k][part])

                @pl.when(has_below & has_above)
                def _():
                    kept = jnp.where(take_down, down_in[k][part], own[k][part])
                    out[k][part] = jnp.where(take_up, up_in[k][part], kept)

            offset += number

    def each_piece(index, action):
        offset = 0
        for k, (number, rows) in enumerate(pieces):

            @pl.when((index >= offset) & (index < offset + number))
            def _(k=k, rows=rows, offset=offset):
                action(k, pl.ds(pl.multiple_of((index - offset) * rows, rows), rows), index)

            offset += number

    def await_own(k, part, index):
        pltpu.make_async_copy(source[k].at[part], own[k].at[part], loaded.at[index]).wait()

    def store(k, part, index):
        pltpu.make_async_copy(out[k].at[part], result[k].at[part], stored.at[k]).start()

    def step(t, carry):
        up_index = t - chip * lag
        down_index = t - (chips - 1 - chip) * lag
        each_piece(jnp.maximum(up_index, down_index), await_own)
        stream(
            up_index, chip == 0, chip == chips - 1, above, start_up, up_in, up_out, up_sent, up_got
        )
        stream(
            down_index,
            chip == chips - 1,
            chip == 0,
            below,
            start_down,
            down_in,
            down_out,
            down_sent,
            down_got,
        )
        settled = jnp.minimum(up_index, down_index)
        settle(settled)
        each_piece(settled - 1, store)
        return carry

    lax.fori_loop(0, total + (chips - 1) * lag + 1, step, 0)

    for k in range(count):
        pltpu.make_async_copy(out[k], result[k], stored.at[k]).wait()

        @pl.when(has_above)
        def _(k=k):
            pltpu.make_async_copy(up_in[k], up_in[k], up_sent.at[k]).wait()

        @pl.when(has_below)
        def _(k=k):
            pltpu.make_async_copy(down_in[k], down_in[k], down_sent.at[k]).wait()


def conveyed(arrays, place, this_round, lag, piece_bytes):
    chips = place.shape[0]
    pieces = []
    for array in arrays:
        row_bytes = array.shape[1] * 2
        rows = max(16, piece_bytes // row_bytes // 16 * 16)
        while array.shape[0] % rows:
            rows -= 16
        pieces.append((array.shape[0] // rows, rows))
    total = sum(number for number, _ in pieces)
    whole = [pltpu.VMEM(array.shape, array.dtype) for array in arrays]
    moved = sum(array.size * 2 for array in arrays)
    in_place = pl.BlockSpec(memory_space=pl.ANY)
    return pl.pallas_call(
        functools.partial(conveyor_kernel, chips, lag, tuple(pieces), this_round),
        out_shape=[jax.ShapeDtypeStruct(array.shape, array.dtype) for array in arrays],
        in_specs=[pl.BlockSpec(memory_space=pltpu.SMEM)] + [in_place] * len(arrays),
        out_specs=[in_place] * len(arrays),
        scratch_shapes=whole * 6
        + [
            pltpu.SemaphoreType.DMA((total,)),
            pltpu.SemaphoreType.DMA((len(arrays),)),
            pltpu.SemaphoreType.DMA((len(arrays),)),
            pltpu.SemaphoreType.DMA((len(arrays),)),
            pltpu.SemaphoreType.DMA((total,)),
            pltpu.SemaphoreType.DMA((total,)),
        ],
        compiler_params=pltpu.CompilerParams(
            collective_id=1 + this_round, has_side_effects=True, vmem_limit_bytes=62 << 20
        ),
        cost_estimate=pl.CostEstimate(
            flops=100 * moved, bytes_accessed=2 * moved, transcendentals=0
        ),
    )(place, *arrays)


def first_journey(arrays, place):
    flat = [array.reshape(-1, array.shape[-1]) for array in arrays]
    return flat, tuple(conveyed(flat, place, 0, LAG, PIECE))


def further_journeys(flat, result, place, need):
    chips = place.shape[0]
    chip = lax.axis_index("expert") // 2

    def rounds_from(this_round, before):
        if this_round == chips // 2:
            return before

        def further(before):
            _, _, take_up, take_down = journey_flags(
                [place[i] for i in range(chips)], chip, this_round
            )
            moved = conveyed(flat, place, this_round, LAG, PIECE)
            merged = tuple(
                jnp.where(take_up | take_down, new, old) for new, old in zip(moved, before)
            )
            return rounds_from(this_round + 1, merged)

        return lax.cond(need > this_round, further, lambda before: before, before)

    return rounds_from(1, result)


def whole_step(
    tokens,
    cotangent,
    norm_gain,
    first_ids,
    first_gates,
    second_ids,
    second_gates,
    new_slot,
    inner_weight,
    outer_weight,
    inner_mean,
    outer_mean,
    inner_square,
    outer_square,
):
    pair_count = new_slot.shape[1]
    rows_here = tokens.shape[1]
    top_count = first_ids.shape[2]
    usual = rows_here * top_count // pair_count
    capacity = min(rows_here, usual + usual // 8)
    rows = pair_count * capacity
    chip = lax.axis_index("expert") // 2
    ahead = (jnp.arange(pair_count, dtype=jnp.int32) - chip) % pair_count
    need = jnp.max(crossing_counts(new_slot[0]))
    for distance in range(1, lax.axis_size("pipe")):
        need = jnp.maximum(
            need, jnp.max(crossing_counts(passed_along(new_slot, "pipe", distance)[0]))
        )
    inner_parts = gathered_parts(inner_weight[0, 0].astype(jnp.bfloat16))
    outer_parts = gathered_parts(outer_weight[0, 0].astype(jnp.bfloat16))
    gain_row = turned(norm_gain[0])
    token_rows = turned(tokens[0])
    slots = slot_index(first_ids[0], ahead, capacity)
    packed = pack_rows(normed(token_rows, gain_row), slots, rows).astype(jnp.bfloat16)
    arrived = dispatched(packed, pair_count)
    gates = first_gates[0].T
    slot_gates = jnp.sum(selection(slots, gates, rows), axis=1, keepdims=True)
    grad_packed = (pack_rows(turned(cotangent[0]), slots, rows) * slot_gates).astype(jnp.bfloat16)
    grad_arrived = dispatched(grad_packed, pair_count)
    half_out, *kept = half_forward(arrived, inner_parts, outer_parts)
    activity, gate_proj, up_proj = lax.optimization_barrier(kept)
    grad_inner, grad_outer = half_backward(
        arrived, grad_arrived, outer_parts, activity, gate_proj, up_proj
    )
    sum_inner = summed_own(grad_inner)
    sum_outer = summed_own(grad_outer)
    first_out = returned_rows(token_rows, half_out, slots, gates, pair_count)
    shifted = passed_along(first_out, "pipe", 1)
    new_inner, new_mean_in, new_square_in = adam_step(
        inner_weight[0, 0], inner_mean[0, 0], inner_square[0, 0], sum_inner
    )
    new_outer, new_mean_out, new_square_out = adam_step(
        outer_weight[0, 0], outer_mean[0, 0], outer_square[0, 0], sum_outer
    )
    low_inner, low_outer = for_sending((new_inner, new_outer))
    inner_two, outer_two = gathered_parts(low_inner), gathered_parts(low_outer)
    slots_two = slot_index(second_ids[0], ahead, capacity)
    packed_two = pack_rows(normed(shifted, gain_row), slots_two, rows).astype(jnp.bfloat16)
    stepped = (low_outer, new_mean_out, new_square_out, low_inner, new_mean_in, new_square_in)
    packed_two, need = lax.optimization_barrier((packed_two, need))
    arrived_two = dispatched(packed_two, pair_count)
    stepped, arrived_two = lax.optimization_barrier((stepped, arrived_two))
    flat, moved = first_journey(stepped, new_slot[0])
    moved, arrived_two, inner_two, outer_two = lax.optimization_barrier(
        (moved, arrived_two, inner_two, outer_two)
    )
    half_two = half_forward(arrived_two, inner_two, outer_two)[0]
    second_out = turned(
        returned_rows(shifted, half_two, slots_two, second_gates[0].T, pair_count),
        back=True,
    )
    moved = further_journeys(flat, moved, new_slot[0], need)
    moved = [
        jnp.where(need < 0, 0.0, array.astype(jnp.float32)).astype(
            jnp.bfloat16 if position % 3 else jnp.float32
        )
        for position, array in enumerate(moved)
    ]
    outer_shape, inner_shape = outer_weight.shape, inner_weight.shape
    return (
        second_out[None],
        moved[3].reshape(inner_shape),
        moved[0].reshape(outer_shape),
        moved[4].reshape(inner_shape),
        moved[1].reshape(outer_shape),
        moved[5].reshape(inner_shape),
        moved[2].reshape(outer_shape),
    )


def solution(mesh):
    return jax.shard_map(
        whole_step,
        mesh=mesh,
        in_specs=(
            P("pipe", ("expert", "dp"), None),
            P("pipe", ("expert", "dp"), None),
            P("pipe", None),
            P("pipe", ("expert", "dp"), None),
            P("pipe", ("expert", "dp"), None),
            P("pipe", ("expert", "dp"), None),
            P("pipe", ("expert", "dp"), None),
            P("pipe", None),
            P("pipe", "expert", None, "dp", None),
            P("pipe", "expert", None, "dp"),
            P("pipe", "expert", None, "dp", None),
            P("pipe", "expert", None, "dp"),
            P("pipe", "expert", None, "dp", None),
            P("pipe", "expert", None, "dp"),
        ),
        out_specs=(
            P("pipe", ("expert", "dp"), None),
            P("pipe", "expert", None, "dp", None),
            P("pipe", "expert", None, "dp"),
            P("pipe", "expert", None, "dp", None),
            P("pipe", "expert", None, "dp"),
            P("pipe", "expert", None, "dp", None),
            P("pipe", "expert", None, "dp"),
        ),
        check_vma=False,
    )
```

```python
import functools

import jax
import jax.numpy as jnp
from jax import lax
from jax.experimental import pallas as pl
from jax.experimental.pallas import tpu as pltpu
from jax.sharding import PartitionSpec as P


MESH = pl.DeviceIdType.MESH

norm_eps = 1e-06
learn_rate = 0.001
beta_one = 0.9
beta_two = 0.95
adam_eps = 1e-08
bias_one = 0.999973438601112
bias_two = 0.994079470779667
LAG = 2
PIECE = 98304


def for_sending(array):

    def short(part):
        return part.astype(jnp.bfloat16) if part.dtype == jnp.float32 else part

    return jax.tree.map(short, array)


def passed_along(block, axis, distance):
    devices = range(lax.axis_size(axis))
    route = [((i - distance) % len(devices), i) for i in devices]
    return lax.ppermute(block, axis, route)


def normed(values, gain_row):
    widened = values.astype(jnp.float32)
    inverse_rms = lax.rsqrt(jnp.mean(widened * widened, axis=-1, keepdims=True) + norm_eps)
    return (widened * inverse_rms * gain_row).astype(jnp.bfloat16)


def silu_parts(gate_proj):
    logistic = jax.nn.sigmoid(gate_proj)
    return (gate_proj * logistic, logistic * (1.0 + gate_proj * (1.0 - logistic)))


def columns(rows, part, parts):
    width = rows.shape[-1] // parts
    return rows[..., part * width : (part + 1) * width]


def half_forward(token_rows, inner_parts, outer_parts):
    count = len(inner_parts)

    def projected(which):
        return sum(
            jnp.dot(
                columns(token_rows, part, count),
                inner_parts[part][which],
                preferred_element_type=jnp.float32,
            )
            for part in range(count)
        )

    gate_proj, up_proj = projected(0), projected(1)
    activity = (silu_parts(gate_proj)[0] * up_proj).astype(jnp.bfloat16)

    def half_out(rows):
        return jnp.concatenate(
            [
                jnp.dot(rows, outer, preferred_element_type=jnp.float32).astype(jnp.bfloat16)
                for outer in outer_parts
            ],
            axis=-1,
        )

    middle = activity.shape[0] // 2
    for_partner = half_out(activity[middle:])
    for_own = half_out(activity[:middle])
    return ((for_own, for_partner), activity, gate_proj, up_proj)


def half_backward(token_rows, grad_rows, outer_parts, activity, gate_proj, up_proj):
    count = len(outer_parts)

    def outer_part(part):
        return jnp.dot(
            activity.T, columns(grad_rows, part, count), preferred_element_type=jnp.float32
        ).astype(jnp.bfloat16)

    grad_outer = [outer_part(part) for part in range(count)]
    d_active = sum(
        jnp.dot(
            columns(grad_rows, part, count),
            outer_parts[part].T,
            preferred_element_type=jnp.float32,
        )
        for part in range(count)
    )
    swish_value, swish_slope = silu_parts(gate_proj)
    d_gate = (d_active * up_proj * swish_slope).astype(jnp.bfloat16)
    d_upper = (d_active * swish_value).astype(jnp.bfloat16)

    def inner_part(part):
        rows = columns(token_rows, part, count).T
        return jnp.stack(
            [
                jnp.dot(rows, d_gate, preferred_element_type=jnp.float32).astype(jnp.bfloat16),
                jnp.dot(rows, d_upper, preferred_element_type=jnp.float32).astype(jnp.bfloat16),
            ]
        )

    return ([inner_part(part) for part in range(count)], grad_outer)


def slot_index(ids, target, capacity):
    count, tokens = target.shape[0], ids.shape[0]
    experts = jnp.arange(count, dtype=jnp.int32)[None, :, None]
    chosen = (ids.T[:, None, :] == experts).astype(jnp.bfloat16)
    places = jnp.arange(tokens, dtype=jnp.int32)
    earlier = (places[:, None] < places[None, :]).astype(jnp.bfloat16)
    ranks = jnp.dot(
        chosen.reshape(-1, tokens), earlier, preferred_element_type=jnp.float32
    ).reshape(chosen.shape)
    chosen = chosen.astype(jnp.float32)
    totals = jnp.sum(chosen, axis=2, keepdims=True)
    before = jnp.cumsum(totals, axis=0) - totals
    starts = (target * capacity).astype(jnp.float32)[None, :, None]
    return jnp.sum(chosen * (starts + before + ranks), axis=1).astype(jnp.int32)


def selection(slots, values, total_slots):
    positions = jnp.arange(total_slots, dtype=jnp.int32)
    result = jnp.zeros((total_slots, slots.shape[1]), jnp.float32)
    for choice in range(slots.shape[0]):
        result = result + jnp.where(
            slots[choice][None, :] == positions[:, None], values[choice][None, :], 0.0
        )
    return result


def across_chips(blocks):
    devices = lax.axis_size("expert")
    arrived = [blocks[0]]
    for distance in range(1, len(blocks)):
        route = [(i, (i + 2 * distance) % devices) for i in range(devices)]
        arrived.append(lax.ppermute(blocks[distance], "expert", route))
    return arrived


def back_across_chips(blocks):
    devices = lax.axis_size("expert")
    arrived = [blocks[0]]
    for distance in range(1, len(blocks)):
        route = [(i, (i - 2 * distance) % devices) for i in range(devices)]
        arrived.append(lax.ppermute(blocks[distance], "expert", route))
    return arrived


def to_partner(block):
    devices = range(lax.axis_size("expert"))
    return lax.ppermute(block, "expert", [(i, i ^ 1) for i in devices])


def blocks_of(rows, count):
    size = rows.shape[0] // count
    return [rows[k * size : (k + 1) * size] for k in range(count)]


def dispatched(packed, pair_count):
    own = jnp.concatenate(across_chips(blocks_of(packed, pair_count)), axis=0)
    return jnp.concatenate([own, to_partner(own)], axis=0)


def from_ahead(block, axis, distance):
    return passed_along(block, axis, lax.axis_size(axis) - distance)


def turned(rows, back=False):
    share = rows.shape[-1] // lax.axis_size("dp")
    own = lax.axis_index("dp") * share
    return jnp.roll(rows, own if back else -own, axis=-1)


def gathered_parts(block):
    return [block] + [
        from_ahead(block, "dp", distance) for distance in range(1, lax.axis_size("dp"))
    ]


def summed_own(parts):
    total = parts[0].astype(jnp.float32)
    for distance in range(1, len(parts)):
        total = total + passed_along(parts[distance], "dp", distance).astype(jnp.float32)
    return total


def pack_rows(normal, slots, rows):
    picker = selection(slots, jnp.ones(slots.shape, jnp.float32), rows).astype(jnp.bfloat16)
    packed = jnp.dot(picker, normal, preferred_element_type=jnp.float32)
    return packed


def returned_rows(token_rows, half_out, slots, gates, pair_count):
    for_own, for_partner = half_out
    rows = for_own.shape[0]
    other = to_partner(for_partner)
    summed = (for_own.astype(jnp.float32) + other.astype(jnp.float32)).astype(jnp.bfloat16)
    back = jnp.concatenate(back_across_chips(blocks_of(summed, pair_count)), axis=0)
    weighting = selection(slots, gates, rows)
    high = weighting.astype(jnp.bfloat16)
    rest = (weighting - high.astype(jnp.float32)).astype(jnp.bfloat16)

    def weighted(share):
        return lax.dot_general(
            share, back, (((0,), (0,)), ((), ())), preferred_element_type=jnp.float32
        )

    mixed = weighted(high) + weighted(rest)
    return (token_rows.astype(jnp.float32) + mixed).astype(jnp.bfloat16)


def adam_step(weight, mean, square, grads):
    mean_new = (beta_one * mean.astype(jnp.float32) + (1.0 - beta_one) * grads).astype(jnp.bfloat16)
    square_new = (beta_two * square.astype(jnp.float32) + (1.0 - beta_two) * grads * grads).astype(
        jnp.bfloat16
    )
    mean_wide = lax.optimization_barrier(mean_new).astype(jnp.float32)
    square_wide = lax.optimization_barrier(square_new).astype(jnp.float32)
    update = mean_wide / bias_one / (jnp.sqrt(square_wide / bias_two) + adam_eps)
    return (weight - learn_rate * update, mean_new, square_new)


def crossing_counts(place):
    count = place.shape[-1]
    own = jnp.arange(count, dtype=jnp.int32)
    link = own[:-1, None]
    crosses = (own[None, :] <= link) & (place[..., None, :] > link)
    return jnp.sum(crosses.astype(jnp.int32), axis=-1)


def journey_flags(places, chip, this_round):
    count = len(places)

    def coloured(order, upward):
        moves = [(places[i] > i) if upward else (places[i] < i) for i in range(count)]
        rounds = [None] * count
        for position, item in enumerate(order):
            chosen = jnp.int32(0)
            for r in reversed(range(count // 2)):
                busy = jnp.bool_(False)
                for before in order[:position]:
                    passes = (places[before] > item) if upward else (places[before] < item)
                    busy = busy | (moves[before] & passes & (rounds[before] == r))
                chosen = jnp.where(busy, chosen, r)
            rounds[item] = chosen
        active = [moves[i] & (rounds[i] == this_round) for i in range(count)]
        starts, ends = jnp.bool_(False), jnp.bool_(False)
        for i in range(count):
            starts = starts | (active[i] & (chip == i))
            ends = ends | (active[i] & (places[i] == chip))
        return starts, ends

    start_up, take_up = coloured(list(range(count)), True)
    start_down, take_down = coloured(list(reversed(range(count))), False)
    return start_up, start_down, take_up, take_down


def conveyor_kernel(chips, lag, pieces, this_round, places, *refs):
    count = len(pieces)
    source = refs[:count]
    prior = ()
    if this_round:
        prior, refs = refs[count : 2 * count], refs[:count] + refs[2 * count :]
    result = refs[count : 2 * count]
    own = refs[2 * count : 3 * count]
    out = refs[3 * count : 4 * count]
    up_in = refs[4 * count : 5 * count]
    down_in = refs[5 * count : 6 * count]
    up_out = refs[6 * count : 7 * count]
    down_out = refs[7 * count : 8 * count]
    loaded, stored, up_sent, down_sent, up_got, down_got, *primed = refs[8 * count :]
    kept = out if prior else own
    place = lax.axis_index("expert")
    chip = place // 2
    above, below = {"expert": place + 2}, {"expert": place - 2}
    has_above, has_below = chip < chips - 1, chip > 0

    offset = 0
    for k, (number, rows) in enumerate(pieces):

        def load(i, carry, k=k, rows=rows, offset=offset):
            part = pl.ds(pl.multiple_of(i * rows, rows), rows)
            pltpu.make_async_copy(source[k].at[part], own[k].at[part], loaded.at[offset + i]).start()
            if prior:
                pltpu.make_async_copy(
                    prior[k].at[part], out[k].at[part], primed[0].at[offset + i]
                ).start()
            return carry

        lax.fori_loop(0, number, load, 0)
        offset += number

    barrier = pltpu.get_barrier_semaphore()

    @pl.when(has_above)
    def _():
        pl.semaphore_signal(barrier, inc=1, device_id=above, device_id_type=MESH)

    @pl.when(has_below)
    def _():
        pl.semaphore_signal(barrier, inc=1, device_id=below, device_id_type=MESH)

    pl.semaphore_wait(barrier, has_above.astype(jnp.int32) + has_below.astype(jnp.int32))

    start_up, start_down, take_up, take_down = journey_flags(
        [places[i] for i in range(chips)], chip, this_round
    )
    total = sum(number for number, _ in pieces)

    def send(block, target, sent, got, k, index, device):
        pltpu.make_async_remote_copy(
            src_ref=block,
            dst_ref=target,
            send_sem=sent.at[k],
            recv_sem=got.at[index],
            device_id=device,
            device_id_type=MESH,
        ).start()

    def stream(index, first, last, onward, starting, arrived, leaving, sent, got):
        offset = 0
        for k, (number, rows) in enumerate(pieces):

            @pl.when((index >= offset) & (index < offset + number))
            def _(k=k, rows=rows, offset=offset):
                part = pl.ds(pl.multiple_of((index - offset) * rows, rows), rows)

                @pl.when(first)
                def _():
                    send(own[k].at[part], arrived[k].at[part], sent, got, k, index, onward)

                @pl.when(jnp.logical_not(first))
                def _():
                    pltpu.make_async_copy(
                        arrived[k].at[part], arrived[k].at[part], got.at[index]
                    ).wait()

                    @pl.when(jnp.logical_not(last))
                    def _():
                        leaving[k][part] = jnp.where(starting, own[k][part], arrived[k][part])
                        send(leaving[k].at[part], arrived[k].at[part], sent, got, k, index, onward)

            offset += number

    def settle(index):
        offset = 0
        for k, (number, rows) in enumerate(pieces):

            @pl.when((index >= offset) & (index < offset + number))
            def _(k=k, rows=rows, offset=offset):
                part = pl.ds(pl.multiple_of((index - offset) * rows, rows), rows)
                if prior:
                    pltpu.make_async_copy(
                        prior[k].at[part], out[k].at[part], primed[0].at[index]
                    ).wait()

                @pl.when(jnp.logical_not(has_below))
                def _():
                    out[k][part] = jnp.where(take_down, down_in[k][part], kept[k][part])

                @pl.when(jnp.logical_not(has_above))
                def _():
                    out[k][part] = jnp.where(take_up, up_in[k][part], kept[k][part])

                @pl.when(has_below & has_above)
                def _():
                    other = jnp.where(take_down, down_in[k][part], kept[k][part])
                    out[k][part] = jnp.where(take_up, up_in[k][part], other)

            offset += number

    def each_piece(index, action):
        offset = 0
        for k, (number, rows) in enumerate(pieces):

            @pl.when((index >= offset) & (index < offset + number))
            def _(k=k, rows=rows, offset=offset):
                action(k, pl.ds(pl.multiple_of((index - offset) * rows, rows), rows), index)

            offset += number

    def await_own(k, part, index):
        pltpu.make_async_copy(source[k].at[part], own[k].at[part], loaded.at[index]).wait()

    def store(k, part, index):
        pltpu.make_async_copy(out[k].at[part], result[k].at[part], stored.at[k]).start()

    def step(t, carry):
        up_index = t - chip * lag
        down_index = t - (chips - 1 - chip) * lag
        each_piece(jnp.maximum(up_index, down_index), await_own)
        stream(
            up_index, chip == 0, chip == chips - 1, above, start_up, up_in, up_out, up_sent, up_got
        )
        stream(
            down_index,
            chip == chips - 1,
            chip == 0,
            below,
            start_down,
            down_in,
            down_out,
            down_sent,
            down_got,
        )
        settled = jnp.minimum(up_index, down_index)
        settle(settled)
        each_piece(settled - 1, store)
        return carry

    lax.fori_loop(0, total + (chips - 1) * lag + 1, step, 0)

    for k in range(count):
        pltpu.make_async_copy(out[k], result[k], stored.at[k]).wait()

        @pl.when(has_above)
        def _(k=k):
            pltpu.make_async_copy(up_in[k], up_in[k], up_sent.at[k]).wait()

        @pl.when(has_below)
        def _(k=k):
            pltpu.make_async_copy(down_in[k], down_in[k], down_sent.at[k]).wait()


def conveyed(arrays, place, this_round, lag, piece_bytes, before=()):
    chips = place.shape[0]
    pieces = []
    for array in arrays:
        row_bytes = array.shape[1] * 2
        rows = max(16, piece_bytes // row_bytes // 16 * 16)
        while array.shape[0] % rows:
            rows -= 16
        pieces.append((array.shape[0] // rows, rows))
    total = sum(number for number, _ in pieces)
    whole = [pltpu.VMEM(array.shape, array.dtype) for array in arrays]
    moved = sum(array.size * 2 for array in arrays)
    in_place = pl.BlockSpec(memory_space=pl.ANY)
    return pl.pallas_call(
        functools.partial(conveyor_kernel, chips, lag, tuple(pieces), this_round),
        out_shape=[jax.ShapeDtypeStruct(array.shape, array.dtype) for array in arrays],
        in_specs=[pl.BlockSpec(memory_space=pltpu.SMEM)] + [in_place] * len(arrays + list(before)),
        out_specs=[in_place] * len(arrays),
        scratch_shapes=whole * 6
        + [
            pltpu.SemaphoreType.DMA((total,)),
            pltpu.SemaphoreType.DMA((len(arrays),)),
            pltpu.SemaphoreType.DMA((len(arrays),)),
            pltpu.SemaphoreType.DMA((len(arrays),)),
            pltpu.SemaphoreType.DMA((total,)),
            pltpu.SemaphoreType.DMA((total,)),
        ]
        + [pltpu.SemaphoreType.DMA((total,))] * bool(before),
        compiler_params=pltpu.CompilerParams(
            collective_id=1 + this_round, has_side_effects=True, vmem_limit_bytes=62 << 20
        ),
        cost_estimate=pl.CostEstimate(
            flops=100 * moved, bytes_accessed=2 * moved, transcendentals=0
        ),
    )(place, *arrays, *before)


def first_journey(arrays, place):
    flat = [array.reshape(-1, array.shape[-1]) for array in arrays]
    return flat, tuple(conveyed(flat, place, 0, LAG, PIECE))


def further_journeys(flat, result, place, need):
    chips = place.shape[0]

    def rounds_from(this_round, before):
        if this_round == chips // 2:
            return before

        def further(before):
            merged = conveyed(flat, place, this_round, LAG, PIECE, before)
            return rounds_from(this_round + 1, tuple(merged))

        return lax.cond(need > this_round, further, lambda before: before, before)

    return rounds_from(1, result)


def whole_step(
    tokens,
    cotangent,
    norm_gain,
    first_ids,
    first_gates,
    second_ids,
    second_gates,
    new_slot,
    inner_weight,
    outer_weight,
    inner_mean,
    outer_mean,
    inner_square,
    outer_square,
):
    pair_count = new_slot.shape[1]
    rows_here = tokens.shape[1]
    top_count = first_ids.shape[2]
    usual = rows_here * top_count // pair_count
    capacity = min(rows_here, usual + usual // 8)
    rows = pair_count * capacity
    chip = lax.axis_index("expert") // 2
    ahead = (jnp.arange(pair_count, dtype=jnp.int32) - chip) % pair_count
    need = jnp.max(crossing_counts(new_slot[0]))
    for distance in range(1, lax.axis_size("pipe")):
        need = jnp.maximum(
            need, jnp.max(crossing_counts(passed_along(new_slot, "pipe", distance)[0]))
        )
    inner_parts = gathered_parts(inner_weight[0, 0].astype(jnp.bfloat16))
    outer_parts = gathered_parts(outer_weight[0, 0].astype(jnp.bfloat16))
    gain_row = turned(norm_gain[0])
    token_rows = turned(tokens[0])
    slots = slot_index(first_ids[0], ahead, capacity)
    packed = pack_rows(normed(token_rows, gain_row), slots, rows).astype(jnp.bfloat16)
    arrived = dispatched(packed, pair_count)
    gates = first_gates[0].T
    slot_gates = jnp.sum(selection(slots, gates, rows), axis=1, keepdims=True)
    grad_packed = (pack_rows(turned(cotangent[0]), slots, rows) * slot_gates).astype(jnp.bfloat16)
    grad_arrived = dispatched(grad_packed, pair_count)
    half_out, *kept = half_forward(arrived, inner_parts, outer_parts)
    activity, gate_proj, up_proj = lax.optimization_barrier(kept)
    grad_inner, grad_outer = half_backward(
        arrived, grad_arrived, outer_parts, activity, gate_proj, up_proj
    )
    sum_inner = summed_own(grad_inner)
    sum_outer = summed_own(grad_outer)
    first_out = returned_rows(token_rows, half_out, slots, gates, pair_count)
    shifted = passed_along(first_out, "pipe", 1)
    new_inner, new_mean_in, new_square_in = adam_step(
        inner_weight[0, 0], inner_mean[0, 0], inner_square[0, 0], sum_inner
    )
    new_outer, new_mean_out, new_square_out = adam_step(
        outer_weight[0, 0], outer_mean[0, 0], outer_square[0, 0], sum_outer
    )
    low_inner, low_outer = for_sending((new_inner, new_outer))
    inner_two, outer_two = gathered_parts(low_inner), gathered_parts(low_outer)
    slots_two = slot_index(second_ids[0], ahead, capacity)
    packed_two = pack_rows(normed(shifted, gain_row), slots_two, rows).astype(jnp.bfloat16)
    stepped = (low_outer, new_mean_out, new_square_out, low_inner, new_mean_in, new_square_in)
    packed_two, need = lax.optimization_barrier((packed_two, need))
    arrived_two = dispatched(packed_two, pair_count)
    stepped, arrived_two = lax.optimization_barrier((stepped, arrived_two))
    flat, moved = first_journey(stepped, new_slot[0])
    moved, arrived_two, inner_two, outer_two = lax.optimization_barrier(
        (moved, arrived_two, inner_two, outer_two)
    )
    half_two = half_forward(arrived_two, inner_two, outer_two)[0]
    second_out = turned(
        returned_rows(shifted, half_two, slots_two, second_gates[0].T, pair_count),
        back=True,
    )
    moved = further_journeys(flat, moved, new_slot[0], need)
    moved = [
        jnp.where(need < 0, 0.0, array.astype(jnp.float32)).astype(
            jnp.bfloat16 if position % 3 else jnp.float32
        )
        for position, array in enumerate(moved)
    ]
    outer_shape, inner_shape = outer_weight.shape, inner_weight.shape
    return (
        second_out[None],
        moved[3].reshape(inner_shape),
        moved[0].reshape(outer_shape),
        moved[4].reshape(inner_shape),
        moved[1].reshape(outer_shape),
        moved[5].reshape(inner_shape),
        moved[2].reshape(outer_shape),
    )


def solution(mesh):
    return jax.shard_map(
        whole_step,
        mesh=mesh,
        in_specs=(
            P("pipe", ("expert", "dp"), None),
            P("pipe", ("expert", "dp"), None),
            P("pipe", None),
            P("pipe", ("expert", "dp"), None),
            P("pipe", ("expert", "dp"), None),
            P("pipe", ("expert", "dp"), None),
            P("pipe", ("expert", "dp"), None),
            P("pipe", None),
            P("pipe", "expert", None, "dp", None),
            P("pipe", "expert", None, "dp"),
            P("pipe", "expert", None, "dp", None),
            P("pipe", "expert", None, "dp"),
            P("pipe", "expert", None, "dp", None),
            P("pipe", "expert", None, "dp"),
        ),
        out_specs=(
            P("pipe", ("expert", "dp"), None),
            P("pipe", "expert", None, "dp", None),
            P("pipe", "expert", None, "dp"),
            P("pipe", "expert", None, "dp", None),
            P("pipe", "expert", None, "dp"),
            P("pipe", "expert", None, "dp", None),
            P("pipe", "expert", None, "dp"),
        ),
        check_vma=False,
    )
```
